256 devices in a mesh: gx: 8 (over z), gy: 32 (over y, x, core).
Axes of the slice: x: 4, y: 4, z: 8, core: 2. Of those that a mesh axis runs over, the one named last changes fastest.
Arguments:
- rhs: float32 [8, 32, 1, 3, 200, 128], P('gx', 'gy'), may hold values from -25 to 25
- stiff_inverse: bfloat16 [8, 32, 1, 1200, 1200], P('gx', 'gy'), may hold values from -2 to 6, as said below
- schur: bfloat16 [8, 32, 1, 1200, 1200], P('gx', 'gy'), may hold values from -2 to 6, as said below
- phi: bfloat16 [8, 32, 1, 24, 1200], P('gx', 'gy'), may hold values from -0.1875 to 0.1875
- coarse_inverse: float32 [1536, 1536], P(('gx', 'gy')), may hold values from -2 to 6, as said below
- incidence: int32 [8, 32, 1, 8], P('gx', 'gy'), may hold values from 0 to 511, as said below
- pairing: int32 [8, 32, 1, 3, 200], P('gx', 'gy'), may hold values from 0 to 199, as said below
Outputs:
- multipliers: float32 [8, 32, 1, 3, 200, 128], P('gx', 'gy')
- reduction: float32 [128], replicated
The draws below stay inside these ranges and needn't reach their ends.
Inputs may be any that keep to these rules, and one draw needn't show every extreme that they name: `stiff_inverse`: each block is symmetric positive definite. `schur`: each block is symmetric positive definite. `coarse_inverse`: symmetric positive definite. `incidence`: the corners of the subdomain grid, periodic in the first two dimensions, under an arbitrary numbering of the 512 nodes: corner c of subdomain (x, y, z) is the grid point (x + c % 2, y + (c // 2) % 2, z + c // 4), and subdomains that share a grid point name the same node. `pairing`: each row over the last dimension is a permutation of 0 to 199.
All inputs are finite; a program needn't handle non-finite values.
Results may differ from the reference program's by a relative error of at most 0.0027.
Values sent between devices are 32-bit elements; how exact they have to be, the bound alone decides.
A program may use at most 64 MiB of HBM per device.

```python
import math
import jax
import jax.numpy as jnp
from jax import lax

ORDER = 1200
FACE = 200
CORNER = 24
LOADS = 128
SUB_DEV = 1
ITERS = 2
GRID_X = 8
GRID_Y = 32
NODES = 512
COARSE = 1536


def definite_block(key, size):
    noise = jax.random.normal(jax.random.fold_in(key, 1), (size, size), jnp.float32)
    coupled = (noise + noise.T) * (0.35 / math.sqrt(2.0 * size))
    diagonal = jax.random.uniform(jax.random.fold_in(key, 2), (size,), jnp.float32, 1.0, 2.0)
    block = coupled + jnp.diag(diagonal)
    return block


def block_stack(key):
    count = GRID_X * GRID_Y * SUB_DEV
    blocks = lax.map(lambda index: definite_block(jax.random.fold_in(key, index), ORDER).astype(jnp.bfloat16), jnp.arange(count))
    return blocks.reshape(GRID_X, GRID_Y, SUB_DEV, ORDER, ORDER)


def draw_stiff_inverse(key, part):
    return block_stack(jax.random.fold_in(key, 11))


def draw_schur(key, part):
    return block_stack(jax.random.fold_in(key, 23))


def draw_coarse_inverse(key, part):
    return definite_block(jax.random.fold_in(key, 37), COARSE)


def draw_rhs(key, part):
    count = GRID_X * GRID_Y * SUB_DEV
    shape = (GRID_X, GRID_Y, SUB_DEV, 3, FACE, LOADS)
    ramp = (jnp.arange(count, dtype=jnp.float32) / max(count - 1, 1)).reshape(GRID_X, GRID_Y, SUB_DEV, 1, 1, 1)
    scale = jnp.exp(math.log(3.0) * ramp)
    base = jax.random.truncated_normal(jax.random.fold_in(key, 63), -4.0, 4.0, shape, jnp.float32)
    return base * scale


def draw_incidence(key, part):
    dof_numbering = jax.random.permutation(jax.random.fold_in(key, 41), NODES).astype(jnp.int32)
    corner = jnp.arange(8, dtype=jnp.int32)
    first = jnp.arange(GRID_X, dtype=jnp.int32)[:, None, None, None] + corner % 2
    second = jnp.arange(GRID_Y, dtype=jnp.int32)[None, :, None, None] + corner // 2 % 2
    third = jnp.arange(SUB_DEV, dtype=jnp.int32)[None, None, :, None] + corner // 4
    node = (first % GRID_X * GRID_Y + second % GRID_Y) * (SUB_DEV + 1) + third
    return dof_numbering[node].astype(jnp.int32)


def draw_pairing(key, part):
    count = GRID_X * GRID_Y * SUB_DEV * 3
    subkeys = jax.random.split(jax.random.fold_in(key, 53), count)
    orderings = jax.vmap(lambda subkey: jax.random.permutation(subkey, FACE))(subkeys).astype(jnp.int32)
    return orderings.reshape(GRID_X, GRID_Y, SUB_DEV, 3, FACE)


def shard_levels(key, extent, pieces, low, high):
    def one(dim, blocks):
        draws = jax.random.uniform(jax.random.fold_in(jax.random.fold_in(key, 6), dim), (blocks,), jnp.float32, low / len(pieces), high / len(pieces))
        return jnp.repeat(jnp.exp(draws), extent[dim] // blocks).reshape((-1,) + (1,) * (len(extent) - dim - 1))

    loudness = one(*pieces[0])
    for cut in pieces[1:]:
        loudness = loudness * one(*cut)
    return loudness


def bell_draw(stream_key, dims, width, limit, pieces=(), held_as=jnp.bfloat16):
    values = jax.random.normal(stream_key, dims, jnp.float32) * width
    if len(pieces) > 0:
        values = shard_levels(stream_key, dims, pieces, -0.22, 0.18) * values
    return jnp.clip(values, min=-limit, max=limit).astype(held_as)


def setup_inputs(seed: int = 0) -> dict:
    key_list = jax.random.split(jax.random.key(seed), 8)
    rhs = draw_rhs(jax.random.fold_in(key_list[7], 71), 0)
    stiff_inverse = draw_stiff_inverse(jax.random.fold_in(key_list[7], 71), 0)
    schur = draw_schur(jax.random.fold_in(key_list[7], 71), 0)
    phi = bell_draw(key_list[3], (GRID_X, GRID_Y, SUB_DEV, CORNER, ORDER), ORDER ** -0.5, 0.1875, ((0, 8), (1, 32)))
    coarse_inverse = draw_coarse_inverse(jax.random.fold_in(key_list[7], 71), 0)
    incidence = draw_incidence(jax.random.fold_in(key_list[7], 71), 0)
    pairing = draw_pairing(jax.random.fold_in(key_list[7], 71), 0)
    return dict(rhs=rhs, stiff_inverse=stiff_inverse, schur=schur, phi=phi, coarse_inverse=coarse_inverse, incidence=incidence, pairing=pairing)


def reference(rhs, stiff_inverse, schur, phi, coarse_inverse, incidence, pairing):
    largest_index = lax.Precision.HIGHEST
    level = jnp.arange(SUB_DEV)[:, None]
    axis_id = jnp.arange(3)[None, :]
    active = jnp.where((level == SUB_DEV - 1) & (axis_id == 2), 0.0, 1.0)
    active = active.astype(jnp.float32)[None, None, :, :, None, None]
    inverse_pairing = jnp.argsort(pairing, axis=-1).astype(jnp.int32)
    coupling_matrix = phi.astype(jnp.float32)
    flat_ids = incidence.reshape(-1).astype(jnp.int32)

    def transpose_jump(values):
        masked = values * active
        moved = jnp.take_along_axis(masked, inverse_pairing[..., None], axis=4)
        lower_x = jnp.roll(moved[:, :, :, 0], 1, axis=0)
        lower_y = jnp.roll(moved[:, :, :, 1], 1, axis=1)
        lower_z = jnp.concatenate([jnp.zeros_like(moved[:, :, :1, 2]), moved[:, :, :-1, 2]], axis=2)
        return jnp.stack([-lower_x, masked[:, :, :, 0], -lower_y, masked[:, :, :, 1], -lower_z, masked[:, :, :, 2]], axis=3)

    def jump_field(field):
        upper_x = jnp.roll(field[:, :, :, 0], -1, axis=0)
        upper_y = jnp.roll(field[:, :, :, 2], -1, axis=1)
        upper_z = jnp.concatenate([field[:, :, 1:, 4], jnp.zeros_like(field[:, :, :1, 4])], axis=2)
        neighbour = jnp.stack([upper_x, upper_y, upper_z], axis=3)
        paired = jnp.take_along_axis(neighbour, pairing[..., None], axis=4)
        higher = jnp.stack([field[:, :, :, 1], field[:, :, :, 3], field[:, :, :, 5]], axis=3)
        return (higher - paired) * active

    def apply_local(matrices, field):
        flat_matrices = matrices.reshape(-1, ORDER, ORDER)
        flat_field = field.reshape(-1, ORDER, LOADS).astype(jnp.bfloat16)
        result = lax.map(lambda both: jnp.dot(both[0], both[1], preferred_element_type=jnp.float32), (flat_matrices, flat_field))
        return result.reshape(GRID_X, GRID_Y, SUB_DEV, 6, FACE, LOADS)

    def operator(values):
        field = transpose_jump(values)
        corner_load = jnp.einsum('xyzco,xyzor->xyzcr', coupling_matrix, field.reshape(GRID_X, GRID_Y, SUB_DEV, ORDER, LOADS), precision=largest_index)
        coarse_load = jax.ops.segment_sum(corner_load.reshape(-1, 3, LOADS), flat_ids, num_segments=NODES).reshape(COARSE, LOADS)
        coarse_solution = jnp.dot(coarse_inverse, coarse_load, precision=largest_index)
        corner_values = coarse_solution.reshape(NODES, 3, LOADS)[flat_ids].reshape(GRID_X, GRID_Y, SUB_DEV, CORNER, LOADS)
        spread_operator = jnp.einsum('xyzco,xyzcr->xyzor', coupling_matrix, corner_values, precision=largest_index)
        displacement = apply_local(stiff_inverse, field) + spread_operator.reshape(GRID_X, GRID_Y, SUB_DEV, 6, FACE, LOADS)
        return jump_field(displacement)

    def precondition(values):
        field = 0.5 * transpose_jump(values)
        return 0.5 * jump_field(apply_local(schur, field))

    def inner_product(left, right):
        return jnp.sum(left * right, axis=(0, 1, 2, 3, 4))

    residual = rhs * active
    multipliers = jnp.zeros_like(residual)
    preconditioned = precondition(residual)
    energy = inner_product(residual, preconditioned)
    start_energy = energy
    direction = preconditioned
    for iteration in range(ITERS):
        product_field = operator(direction)
        alpha = energy / inner_product(direction, product_field)
        multipliers = multipliers + alpha * direction
        residual = residual - alpha * product_field
        preconditioned = precondition(residual)
        energy_next = inner_product(residual, preconditioned)
        if iteration + 1 < ITERS:
            direction = preconditioned + (energy_next / energy) * direction
        energy = energy_next
    return multipliers, energy / start_energy
```

```python
import jax
import jax.numpy as jnp
import numpy as np
from jax import lax
from jax.experimental import pallas as pl
from jax.experimental.pallas import tpu as pltpu
from jax.sharding import PartitionSpec as P

F32, BF16 = jnp.float32, jnp.bfloat16
MESH = pl.DeviceIdType.MESH
HIGHEST = lax.Precision.HIGHEST
FACE, ORDER, LOADS = 200, 1200, 128
SHARED = 4 * FACE
ACTIVE_Z = 0.0
NT = (((1,), (1,)), ((), ()))


def assembly_table():
    table = np.zeros((16, 128, 256), np.float32)
    steps = ((0, 0), (1, 0), (-1, 0), (0, 1), (0, -1))
    for p in range(16):
        x, core = p // 2, p % 2
        for block, (ox, oy) in enumerate(steps):
            for c in range(8):
                gx = (x + ox + c % 2) % 8
                y = core + oy + (c // 2) % 2
                z = c // 4
                for i in range(3):
                    if y == -1:
                        m = 128 * z + 96 + gx * 3 + i
                    else:
                        m = 128 * (y // 2) + (y % 2) * 48 + z * 24 + gx * 3 + i
                    table[p, block * 24 + 3 * c + i, m] = 1.0
        for e in range(8):
            table[p, 120 + e, 120 + e] = 1.0
    return table.reshape(2048, 256)


def loop(low, high, step):
    def body(k, carry):
        step(k)
        return carry

    lax.fori_loop(low, high, body, 0)


def halves(x):
    high = x.astype(BF16)
    return high, (x - high.astype(F32)).astype(BF16)


def stacked(x):
    high = x.astype(BF16).astype(F32)
    return jnp.concatenate([high, x - high], axis=0).astype(BF16)


def iota(shape, dim):
    return lax.broadcasted_iota(jnp.int32, shape, dim)


def dot(a, b):
    return jnp.dot(a, b, preferred_element_type=F32)


def kernel(
    rhs, stiff, schur, phi, coarse, inc, pair, table,
    out, red,
    rv, sm, km, ss, ks, ph, phf, phn, phb, pho, cin, call, pin, pf, pn, at,
    yb, tb, tsb, ts, rx0, rx1, rx2, rx3, rx4, snd,
    y0, t0, w0, d0, yq, tq, wm, dm, ds0, dsm,
    px, phx, phxs, clt, ra, mb, rb, sb, rc, pb, rd, cp, c256, ohp, idt, idr, idm, ids, fb0, fb1, fb2, fb3,
    hsem, xs, xr, ps, pr, fs, fr, is1, ir1, is2, ir2, cs, cr, cps, cpr, gs, gr,
):
    gx, gy = lax.axis_index("gx"), lax.axis_index("gy")
    h, core = gy // 2, gy % 2
    p = gx * 2 + core

    def device(x, y):
        return {"gx": x, "gy": y}

    def ring(q):
        return device(q // 2, 2 * h + q % 2)

    def plane(other):
        return device(gx, 2 * other + core)

    xu, xd = device((gx + 1) % 8, gy), device((gx + 7) % 8, gy)
    yu, yd = device(gx, (gy + 1) % 32), device(gx, (gy + 31) % 32)

    def remote(src, dst, send, recv, target):
        return pltpu.make_async_remote_copy(
            src_ref=src, dst_ref=dst, send_sem=send, recv_sem=recv, device_id=target, device_id_type=MESH
        )

    loads = [(rhs, rv), (pair, pin), (phi, ph), (coarse, cin), (schur, sm), (table, at), (stiff, km)]
    fetch = [pltpu.make_async_copy(a, b, hsem.at[i]) for i, (a, b) in enumerate(loads)]
    for f in fetch:
        f.start()

    barrier = pltpu.get_barrier_semaphore()

    def greet(target):
        pl.semaphore_signal(barrier, inc=1, device_id=target, device_id_type=MESH)

    loop(1, 16, lambda k: greet(ring((p + k) % 16)))
    loop(1, 16, lambda k: greet(plane((h + k) % 16)))
    greet(yu)
    greet(yd)

    fetch[0].wait()
    fetch[1].wait()
    pf[...] = jnp.full((8, 256), -1.0, F32)
    pf[0:3, 0:FACE] = pin[...].astype(F32)
    down = iota((FACE, FACE), 0).astype(F32)
    for a in range(2):
        onto = (pf[a : a + 1, 0:FACE] == down).astype(F32)
        snd[400 * a : 400 * a + FACE, :] = jnp.dot(onto, rv[a], precision=HIGHEST, preferred_element_type=F32)

    lane = iota((8, 128), 1)
    mine = jnp.zeros((8, 128), F32)
    for z in range(2):
        base = core * 48 + z * 24 + gx * 3
        node = jnp.full((8, 128), inc[4 * z], jnp.int32)
        mine = jnp.where((lane >= base) & (lane < base + 3), (3 * node + (lane - base)).astype(F32), mine)
    idt[...] = mine
    idr[p] = mine

    fetch[2].wait()
    phf[...] = ph[...].astype(F32)
    fetch[3].wait()
    call[p, 0:6, :] = cin[...]
    call[p, 6:8, :] = jnp.zeros((2, 1536), F32)

    pl.semaphore_wait(barrier, 32)

    def face_copy(src, dst, turn, face):
        rows = pl.ds(FACE * face, FACE)
        target = (xu, xd, yu, yd)[face]
        return remote(src.at[rows], dst.at[rows], xs.at[turn, face], xr.at[turn, face], target)

    first = [face_copy(snd, rx0, 0, f) for f in (0, 2)]
    for c in first:
        c.start()
    pairs = [remote(pf, pn.at[a], ps.at[a], pr.at[a], (xu, yu)[a]) for a in range(2)]
    for c in pairs:
        c.start()

    def started(me, where, src, dst, send, recv):
        def go(k):
            q = (me + k) % 16
            remote(src(q), dst.at[me], send.at[q], recv.at[me], where(q)).start()

        loop(1, 16, go)

    def ended(me, where, src, dst, send, recv):
        def go(k):
            q = (me + k) % 16
            remote(src(q), dst.at[q], send.at[q], recv.at[q], where(q)).wait_recv()

        def sent(k):
            q = (me + k) % 16
            remote(src(q), dst.at[q], send.at[q], recv.at[q], where(q)).wait_send()

        loop(1, 16, go)
        loop(1, 16, sent)

    id1 = (p, ring, lambda q: idt, idr, is1, ir1)
    started(*id1)

    windows = ((0, 256), (128, 512), (384, 640), (512, 896))
    coupling = []
    for block, target in enumerate((xd, xu, yd, yu)):
        low, high = windows[block]
        coupling.append(
            remote(phf.at[:, low:high], phn.at[block, :, low:high], fs.at[block], fr.at[block], target)
        )
    for c in coupling:
        c.start()

    def row_copy(k):
        x = (gx + k) % 8
        return remote(call.at[p], call.at[p], cs.at[k], cr.at[gx], device(x, gy))

    other = device(gx, 2 * h + 1 - core)
    loop(1, 8, lambda k: row_copy(k).start())
    remote(call.at[p], call.at[p], cps.at[gx], cpr.at[gx], other).start()

    for c in pairs:
        c.wait()
    spare = jnp.full((8, 256), -1.0, F32)
    for a, (up, low) in enumerate(((FACE, 0), (312, 112))):
        wide = jnp.concatenate([pf[...] + 1.0, spare + 1.0], axis=1)
        own = pltpu.roll(wide, up, 1)[a : a + 1, :] - 1.0
        top = (own == iota((FACE, 512), 0).astype(F32)).astype(F32)
        col = jnp.transpose(jnp.concatenate([pn[a]] * 16, axis=0))[0:FACE, a : a + 1]
        bottom = (col + float(low) == iota((FACE, 512), 1).astype(F32)).astype(F32)
        px[a] = jnp.concatenate([top, bottom], axis=0).astype(BF16)

    def sent_rows(matrix, result):
        result[0:400, :] = dot(px[0], matrix[0:512, :]).astype(BF16)
        result[400:800, :] = dot(px[1], matrix[288:800, :]).astype(BF16)

    fetch[4].wait()
    sent_rows(sm, ss)

    for c in coupling:
        c.wait()
    at_lane = iota((24, 896), 1)
    for block in range(4):
        keep = (at_lane >= FACE * block) & (at_lane < FACE * (block + 1))
        phf2 = jnp.where(keep, -phn[block], 0.0)
        phn[block] = phf2
    phb[...] = phn[...].reshape(96, 896).astype(BF16)
    full = iota((24, ORDER), 1)
    zone = jnp.where(full < SHARED, 1.0, jnp.where(full < SHARED + FACE, 0.0, ACTIVE_Z))
    pho[...] = (phf[...] * zone).astype(BF16)
    tsb[800:896, :] = jnp.zeros((96, 256), BF16)

    def put(x, dst, rows):
        high, low = halves(x)
        dst[0:rows, 0:128] = high
        dst[0:rows, 128:256] = low

    def product(matrix, chunks, result):
        def chunk(i):
            rows = pl.ds(pl.multiple_of(i * 400, 400), 400)
            both = dot(matrix[rows, :], yb[...])
            result[rows, :] = both[:, 0:128] + both[:, 128:256]

        loop(0, chunks, chunk)

    def field(u, arrived, scale):
        return jnp.concatenate(
            [
                scale * (u[0:SHARED, :] - arrived[...]),
                jnp.zeros((FACE, LOADS), F32),
                (scale * ACTIVE_Z) * u[SHARED + FACE : ORDER, :],
            ],
            axis=0,
        )

    def total(a, b):
        return jnp.sum(a * b, axis=0, keepdims=True)

    def extras(*rows):
        sub = iota((8, 128), 0)
        tile = jnp.zeros((8, 128), F32)
        for i, row in enumerate(rows):
            tile = jnp.where(sub == i, row, tile)
        return tile

    def faces(src, dst, turn):
        return [face_copy(src, dst, turn, f) for f in range(4)]

    def corner_loads(t, tile):
        put(t[...], tb, ORDER)
        put(ts[...], tsb, SHARED)
        own = dot(pho[...], tb[...])
        nearby = dot(phb[...], tsb[...])
        own = 0.5 * (own[:, 0:128] + own[:, 128:256])
        nearby = 0.5 * (nearby[:, 0:128] + nearby[:, 128:256])
        clt[...] = jnp.transpose(jnp.concatenate([own, nearby, tile], axis=0))

    lane256 = iota((8, 256), 1)
    tail = (lane256 % 128) >= 120

    def coarse(turn, after_send, during_b, during_c):
        g = 4 * turn
        a = (p, ring, lambda q: clt.at[pl.ds(pl.multiple_of(8 * q, 8), 8)], ra.at[turn], gs.at[g], gr.at[g])
        started(*a)
        ra[turn, p] = clt[pl.ds(pl.multiple_of(8 * p, 8), 8), :]
        after_send()
        ended(*a)
        got = jnp.concatenate([ra[turn, i] for i in range(16)], axis=1)
        both = dot(stacked(got), at[...])
        mb[...] = both[0:8] + both[8:16]
        b = (h, plane, lambda q: mb, rb.at[turn], gs.at[g + 1], gr.at[g + 1])
        started(*b)
        rb[turn, h] = mb[...]
        during_b()
        ended(*b)
        pieces, sums = [], jnp.zeros((8, 128), F32)
        for i in range(16):
            here, before, after = rb[turn, i], rb[turn, (i + 15) % 16], rb[turn, (i + 1) % 16]
            sums = sums + here[:, 0:128]
            part = jnp.where(lane < 96, here[:, 0:128] + before[:, 128:256], 0.0)
            part = part + jnp.where((lane >= 48) & (lane < 72), pltpu.roll(after[:, 0:128], 80, 1), 0.0)
            part = part + jnp.where((lane >= 72) & (lane < 96), pltpu.roll(after[:, 128:256], 104, 1), 0.0)
            pieces.append(part)
        four = lax.dot_general(
            stacked(jnp.concatenate(pieces, axis=1)), cp[...], NT, preferred_element_type=F32
        )
        sb[...] = (four[0:8, 0:128] + four[0:8, 128:256]) + (four[8:16, 0:128] + four[8:16, 128:256])
        c = (h, plane, lambda q: sb, rc.at[turn], gs.at[g + 2], gr.at[g + 2])
        started(*c)
        rc[turn, h] = sb[...]
        during_c()
        ended(*c)
        got = jnp.concatenate([rc[turn, i] for i in range(16)], axis=1)
        both = dot(stacked(got), ohp[...])
        picked = jnp.where(tail, jnp.concatenate([sums, sums], axis=1), both[0:8] + both[8:16])
        pb[0] = picked[:, 0:128]
        pb[1] = picked[:, 128:256]
        d = (p, ring, lambda q: pb.at[q % 2], rd.at[turn], gs.at[g + 3], gr.at[g + 3])
        started(*d)
        rd[turn, p] = pb[core]
        ended(*d)
        return jnp.transpose(rd[turn].reshape(128, 128))

    def spread(solved):
        high, low = halves(solved)
        both = jnp.concatenate([high, low], axis=1)
        near, far = dot(phx[...], both), dot(phxs[...], both)
        return near[:, 0:128] + near[:, 128:256], far[:, 0:128] + far[:, 128:256]

    for c in first:
        c.wait()
    zeros = jnp.zeros((FACE, LOADS), F32)
    y0[...] = 0.5 * jnp.concatenate(
        [-rx0[0:FACE, :], rv[0], -rx0[2 * FACE : 3 * FACE, :], rv[1], zeros, ACTIVE_Z * rv[2]], axis=0
    )
    put(y0[...], yb, ORDER)
    product(ss, 2, ts)
    product(sm, 3, t0)
    start_energy = total(y0[...], t0[...])
    fetch[5].wait()
    corner_loads(t0, extras(start_energy))

    turn1 = faces(ts, rx1, 1)

    def setup_early():
        for c in turn1:
            c.start()
        ended(*id1)
        idm[...] = sum([idr[i] for i in range(1, 16)], idr[0])
        started(h, plane, lambda q: idm, ids, is2, ir2)
        ids[h] = idm[...]

        def forward(k):
            x = (gx + k) % 8
            slot = 2 * x + core
            remote(call.at[slot], call.at[slot], cs.at[k], cr.at[x], other).wait_recv()
            remote(call.at[slot], call.at[slot], cps.at[x], cpr.at[x], other).start()

        loop(1, 8, forward)

        e = iota((128, 24), 1)
        c = (e * 11) >> 5
        i = e - 3 * c
        to = ((c >> 1) & 1) * 48 + (c >> 2) * 24 + ((gx + (c & 1)) % 8) * 3 + i
        place = (to == iota((128, 24), 0)).astype(BF16)
        phx[...] = jnp.transpose(dot(place, ph[...])).astype(BF16)
        phxs[0:400, :] = dot(px[0], phx[0:512, :]).astype(BF16)
        phxs[400:800, :] = dot(px[1], phx[288:800, :]).astype(BF16)
        fetch[6].wait()
        sent_rows(km, ks)

    def setup_late():
        loop(1, 8, lambda k: row_copy(k).wait_send())

        def swapped(x):
            slot = 2 * x + 1 - core
            copy = remote(call.at[slot], call.at[slot], cps.at[x], cpr.at[x], other)
            copy.wait_recv()
            copy.wait_send()

        loop(0, 8, swapped)
        high, low = halves(call[...].reshape(128, 1536))
        c256[0:128, :] = high
        c256[128:256, :] = low
        ended(h, plane, lambda q: idm, ids, is2, ir2)
        row = iota((1536, 256), 0)
        lanes = iota((1, 128), 1)

        def columns(j):
            pair_ids = [jnp.where(lanes < 96, ids[2 * j + s][0:1, :], -1.0) for s in range(2)]
            wanted = jnp.concatenate(pair_ids, axis=1).astype(jnp.int32)
            pick = (row == wanted).astype(F32).astype(BF16)
            cp[:, pl.ds(pl.multiple_of(j * 256, 256), 256)] = dot(c256[...], pick).astype(BF16)

        loop(0, 8, columns)
        here, after = ids[h][0:1, :], ids[(h + 1) % 16][0:1, :]
        here8, after8 = ids[h], ids[(h + 1) % 16]
        shifted = jnp.where(lane < 48, pltpu.roll(here8, 80, 1), pltpu.roll(after8, 48, 1))[0:1, :]
        wanted = jnp.concatenate([jnp.where(lanes < 96, v, -1.0) for v in (here, shifted)], axis=1)
        wanted = wanted.astype(jnp.int32)

        def picks(j):
            r = iota((128, 256), 0)
            own = 192 * (r >> 4) + 12 * j + 6 * ((r >> 3) & 1) + (r & 7)
            own = jnp.where((r & 7) < 6, own, -2)
            ohp[pl.ds(pl.multiple_of(j * 128, 128), 128), :] = (own == wanted).astype(F32).astype(BF16)

        loop(0, 16, picks)

    def first_direction():
        for c in turn1:
            c.wait()
        w0[...] = field(t0, rx1, 0.5)
        put(w0[...], yb, ORDER)
        product(ks, 2, ds0)
        product(km, 3, d0)

    solved = coarse(0, setup_early, setup_late, first_direction)
    start_energy = solved[120:121, :]
    near, far = spread(solved)
    ds0[...] = ds0[...] + far
    turn2 = faces(ds0, rx2, 2)
    for c in turn2:
        c.start()
    d0[...] = d0[...] + near
    curvature = total(w0[...], d0[...])

    for c in turn2:
        c.wait()
    yq[...] = field(d0, rx2, 0.5)
    put(yq[...], yb, ORDER)
    product(ss, 2, ts)
    product(sm, 3, tq)
    corner_loads(tq, extras(curvature, total(y0[...], tq[...]), total(yq[...], tq[...])))
    turn3 = faces(ts, rx3, 3)

    def send_third():
        for c in turn3:
            c.start()

    def second_direction():
        for c in turn3:
            c.wait()
        wm[...] = field(tq, rx3, 0.5)
        put(wm[...], yb, ORDER)
        product(ks, 2, dsm)
        product(km, 3, dm)

    solved = coarse(1, send_third, lambda: None, second_direction)
    alpha = start_energy / solved[120:121, :]
    energy = start_energy - 2.0 * alpha * solved[121:122, :] + alpha * alpha * solved[122:123, :]
    ratio = 1.0 + energy / start_energy
    near, far = spread(solved)
    snd[...] = ratio * ds0[...] - alpha * (dsm[...] + far)
    turn4 = faces(snd, rx4, 4)
    for c in turn4:
        c.start()
    d0[...] = ratio * d0[...] - alpha * (dm[...] + near)
    curvature = total(ratio * w0[...] - alpha * wm[...], d0[...])
    y0[...] = y0[...] - alpha * yq[...]

    for c in turn4:
        c.wait()
    yq[...] = field(d0, rx4, 0.5)
    put(yq[...], yb, ORDER)
    product(sm, 3, tq)
    fb0[...] = extras(curvature, total(y0[...], tq[...]), total(yq[...], tq[...]))
    last = (p, ring, lambda q: fb0, fb1, gs.at[8], gr.at[8])
    started(*last)
    fb1[p] = fb0[...]
    ended(*last)
    fb2[...] = sum([fb1[i] for i in range(1, 16)], fb1[0])
    last = (h, plane, lambda q: fb2, fb3, gs.at[9], gr.at[9])
    started(*last)
    fb3[h] = fb2[...]
    ended(*last)
    sums = sum([fb3[i] for i in range(1, 16)], fb3[0])
    step = energy / sums[0:1, :]
    final = energy - 2.0 * step * sums[1:2, :] + step * step * sums[2:3, :]
    red[...] = jnp.broadcast_to(final / start_energy, (8, 128))
    for a in range(3):
        rows = slice(FACE * (2 * a + 1), FACE * (2 * a + 2))
        out[a] = (alpha + step * ratio) * w0[rows, :] - (step * alpha) * wm[rows, :]


def local(rhs, stiff, schur, phi, coarse, inc, pair):
    table = jnp.asarray(assembly_table(), BF16)
    v = pltpu.VMEM
    wide, sent = v((ORDER, LOADS), F32), v((SHARED, LOADS), F32)
    dma = pltpu.SemaphoreType.DMA
    scratch = [
        v((3, FACE, LOADS), F32), v((ORDER, ORDER), BF16), v((ORDER, ORDER), BF16),
        v((SHARED, ORDER), BF16), v((SHARED, ORDER), BF16),
        v((24, ORDER), BF16), v((24, ORDER), F32), v((4, 24, 896), F32), v((96, 896), BF16), v((24, ORDER), BF16),
        v((6, 1536), F32), v((16, 8, 1536), F32), v((3, FACE), jnp.int32), v((8, 256), F32), v((2, 8, 256), F32),
        v((2048, 256), BF16),
        v((ORDER, 256), BF16), v((ORDER, 256), BF16), v((896, 256), BF16),
        sent, sent, sent, sent, sent, sent, sent,
        wide, wide, wide, wide, wide, wide, wide, wide, sent, sent,
        v((2, 400, 512), BF16), v((ORDER, 128), BF16), v((SHARED, 128), BF16),
        v((128, 128), F32), v((2, 16, 8, 128), F32), v((8, 256), F32), v((2, 16, 8, 256), F32),
        v((8, 128), F32), v((2, 16, 8, 128), F32), v((2, 8, 128), F32), v((2, 16, 8, 128), F32),
        v((256, 2048), BF16), v((256, 1536), BF16), v((2048, 256), BF16),
        v((8, 128), F32), v((16, 8, 128), F32), v((8, 128), F32), v((16, 8, 128), F32),
        v((8, 128), F32), v((16, 8, 128), F32), v((8, 128), F32), v((16, 8, 128), F32),
        dma((7,)), dma((5, 4)), dma((5, 4)), dma((2,)), dma((2,)), dma((4,)), dma((4,)),
        dma((16,)), dma((16,)), dma((16,)), dma((16,)),
        dma((8,)), dma((8,)), dma((8,)), dma((8,)), dma((10, 16)), dma((10, 16)),
    ]
    any_space = pl.BlockSpec(memory_space=pl.ANY)
    in_vmem = pl.BlockSpec(memory_space=pltpu.VMEM)
    result, reduction = pl.pallas_call(
        kernel,
        out_shape=(jax.ShapeDtypeStruct((3, FACE, LOADS), F32), jax.ShapeDtypeStruct((8, LOADS), F32)),
        in_specs=[any_space] * 5 + [pl.BlockSpec(memory_space=pltpu.SMEM)] + [any_space] * 2,
        out_specs=(in_vmem, in_vmem),
        scratch_shapes=scratch,
        compiler_params=pltpu.CompilerParams(
            collective_id=0, has_side_effects=True, vmem_limit_bytes=60 * 1024 * 1024
        ),
        name="domain_decomposition",
    )(
        rhs[0, 0, 0], stiff[0, 0, 0], schur[0, 0, 0], phi[0, 0, 0], coarse, inc[0, 0, 0], pair[0, 0, 0], table
    )
    return result[None, None, None], reduction[0]


def solution(mesh):
    four = P("gx", "gy", None, None)
    five = P("gx", "gy", None, None, None)
    six = P("gx", "gy", None, None, None, None)
    return jax.shard_map(
        local,
        mesh=mesh,
        in_specs=(six, five, five, five, P(("gx", "gy"), None), four, five),
        out_specs=(six, P()),
        check_vma=False,
    )
```

```python
import jax
import jax.numpy as jnp
import numpy as np
from jax import lax
from jax.experimental import pallas as pl
from jax.experimental.pallas import tpu as pltpu
from jax.sharding import PartitionSpec as P

F32, BF16 = jnp.float32, jnp.bfloat16
MESH = pl.DeviceIdType.MESH
HIGHEST = lax.Precision.HIGHEST
FACE, ORDER, LOADS = 200, 1200, 128
SHARED = 4 * FACE
ACTIVE_Z = 0.0
NT = (((1,), (1,)), ((), ()))


def assembly_table():
    table = np.zeros((16, 128, 256), np.float32)
    steps = ((0, 0), (1, 0), (-1, 0), (0, 1), (0, -1))
    for p in range(16):
        x, core = p // 2, p % 2
        for block, (ox, oy) in enumerate(steps):
            for c in range(8):
                gx = (x + ox + c % 2) % 8
                y = core + oy + (c // 2) % 2
                z = c // 4
                for i in range(3):
                    if y == -1:
                        m = 128 * z + 96 + gx * 3 + i
                    else:
                        m = 128 * (y // 2) + (y % 2) * 48 + z * 24 + gx * 3 + i
                    table[p, block * 24 + 3 * c + i, m] = 1.0
        for e in range(8):
            table[p, 120 + e, 120 + e] = 1.0
    return table.reshape(2048, 256)


def order_table():
    table = np.zeros((384, 768), np.float32)
    for core in range(2):
        for slot in range(11):
            for y in range(4):
                for z in range(2):
                    for i in range(3):
                        chip, half = divmod(core + 1 + y, 2)
                        lane = chip * 128 + half * 48 + z * 24 + (slot - 1) % 8 * 3 + i
                        table[lane, 384 * core + slot * 24 + y * 6 + z * 3 + i] = 1.0
    return table


def loop(low, high, step):
    def body(k, carry):
        step(k)
        return carry

    lax.fori_loop(low, high, body, 0)


def halves(x):
    high = x.astype(BF16)
    return high, (x - high.astype(F32)).astype(BF16)


def stacked(x):
    high = x.astype(BF16).astype(F32)
    return jnp.concatenate([high, x - high], axis=0).astype(BF16)


def iota(shape, dim):
    return lax.broadcasted_iota(jnp.int32, shape, dim)


def dot(a, b):
    return jnp.dot(a, b, preferred_element_type=F32)


def kernel(
    rhs, stiff, schur, phi, coarse, inc, pair, table, order,
    out, red,
    rv, sm, km, ss, ks, ph, phf, phn, cin, packed, call, pin, pf, pn, at, ot,
    yb, tb, ts, rx0, rx1, rx2, rx3, rx4, snd,
    y0, t0, w0, d0, yp, yq, tq, wm, dm, tp,
    px, pef, pe, pet, big, clt, cl0, cl1, clm,
    ra, mb, rb, sb, rc, pb, rd, cp, c256, ohp, idt, idr, idm, ids, fb0, fb1, fb2, fb3,
    hsem, xs, xr, ps, pr, fs, fr, ns, nr, cs, cr, gs, gr,
):
    gx, gy = lax.axis_index("gx"), lax.axis_index("gy")
    h, core = gy // 2, gy % 2
    p = gx * 2 + core

    def device(x, y):
        return {"gx": x, "gy": y}

    def ring(q):
        return device(q >> 1, 2 * h + (q & 1))

    def plane(other):
        return device(gx, 2 * other + core)

    xu, xd = device((gx + 1) & 7, gy), device((gx + 7) & 7, gy)
    yu, yd = device(gx, (gy + 1) & 31), device(gx, (gy + 31) & 31)

    def remote(src, dst, send, recv, target):
        return pltpu.make_async_remote_copy(
            src_ref=src, dst_ref=dst, send_sem=send, recv_sem=recv, device_id=target, device_id_type=MESH
        )

    loads = [(rhs, rv), (pair, pin), (phi, ph), (coarse, cin), (schur, sm), (table, at), (stiff, km), (order, ot)]
    fetch = [pltpu.make_async_copy(a, b, hsem.at[i]) for i, (a, b) in enumerate(loads)]
    for f in fetch:
        f.start()

    barrier = pltpu.get_barrier_semaphore()

    def greet(target):
        pl.semaphore_signal(barrier, inc=1, device_id=target, device_id_type=MESH)

    loop(1, 16, lambda k: greet(ring((p + k) & 15)))
    loop(1, 16, lambda k: greet(plane((h + k) & 15)))
    greet(yu)
    greet(yd)

    fetch[0].wait()
    fetch[1].wait()
    pf[...] = jnp.full((8, 256), -1000.0, F32)
    for a in range(2):
        pf[a : a + 1, 0:FACE] = pin[a].astype(F32)
    down = iota((FACE, FACE), 0).astype(F32)
    for a in range(2):
        onto = (pf[a : a + 1, 0:FACE] == down).astype(F32)
        snd[400 * a : 400 * a + FACE, :] = jnp.dot(onto, rv[a], precision=HIGHEST, preferred_element_type=F32)

    lane = iota((8, 128), 1)
    mine = jnp.zeros((8, 128), F32)
    for z in range(2):
        base = core * 48 + z * 24 + gx * 3
        node = jnp.full((8, 128), inc[4 * z], jnp.int32)
        mine = jnp.where((lane >= base) & (lane < base + 3), (3 * node + (lane - base)).astype(F32), mine)
    idt[...] = mine
    idr[p] = mine

    fetch[2].wait()
    phf[...] = ph[...].astype(F32)
    fetch[3].wait()
    for k in range(12):
        packed[p, 6 * k : 6 * k + 6, :] = cin[:, 128 * k : 128 * k + 128]
    call[...] = jnp.zeros((16, 8, 1536), F32)

    full = iota((24, ORDER), 1)
    zone = jnp.where(full < SHARED, 1.0, jnp.where(full < SHARED + FACE, 0.0, ACTIVE_Z))
    pef[...] = jnp.zeros((120, ORDER), F32)
    pef[0:24, :] = phf[...] * zone
    r, m = iota((128, 128), 0), iota((128, 128), 1)
    block = (r * 683) >> 14
    e = r - 24 * block
    c = (e * 11) >> 5
    over = 1 + jnp.where(block == 1, 1, 0) - jnp.where(block == 2, 1, 0) + (c & 1)
    up = 1 + jnp.where(block == 3, 1, 0) - jnp.where(block == 4, 1, 0) + ((c >> 1) & 1)
    to = over * 24 + up * 6 + (c >> 2) * 3 + (e - 3 * c)
    place = ((to == m) & (r < 120)).astype(F32).astype(BF16)

    pl.semaphore_wait(barrier, 32)

    def face_copy(src, dst, turn, face):
        rows = pl.ds(FACE * face, FACE)
        return remote(src.at[rows], dst.at[rows], xs.at[turn], xr.at[turn], (xu, xd, yu, yd)[face])

    for a in range(2):
        remote(pf, pn.at[a], ps.at[0], pr.at[0], (xu, yu)[a]).start()
    for f in (0, 2):
        face_copy(snd, rx0, 0, f).start()
    windows = ((0, 384), (128, 512), (384, 768), (512, 896))
    for blk, target in enumerate((xd, xu, yd, yu)):
        low, high = windows[blk]
        remote(phf.at[:, low:high], phn.at[blk, :, low:high], fs.at[0], fr.at[0], target).start()

    def far(step, size):
        return min(step, size - step)

    ring_steps = sorted(((dx, dc) for dx in range(8) for dc in (1, 0)), key=lambda d: -far(d[0], 8))
    ring_others = [2 * ((gx + dx) & 7) + ((core + dc) & 1) for dx, dc in ring_steps if dx or dc]
    plane_steps = sorted(
        ((dy, dx) for dy in range(4) for dx in range(4)), key=lambda d: -far(d[0], 4) - far(d[1], 4)
    )
    plane_others = [4 * (((h >> 2) + dy) & 3) + ((h + dx) & 3) for dy, dx in plane_steps if dy or dx]

    def started(me, where, src, dst, send, recv):
        for q in ring_others if where is ring else plane_others:
            remote(src(q), dst.at[me], send, recv, where(q)).start()

    def ended(dst, send, recv):
        all_blocks = remote(dst.at[0:15], dst.at[0:15], send, recv, xu)
        all_blocks.wait_recv()
        all_blocks.wait_send()

    started(p, ring, lambda q: idt, idr, ns.at[0], nr.at[0])

    other = device(gx, 2 * h + 1 - core)

    def rows_to(slot, target, turn):
        return remote(packed.at[slot], packed.at[slot], cs.at[turn], cr.at[turn], target)

    for k in (1, 7, 2, 6):
        rows_to(p, device((gx + k) & 7, gy), 0).start()
    rows_to(p, other, 2).start()

    def rows_in(count, turn):
        some = packed.at[0:count]
        arrived = remote(some, some, cs.at[turn], cr.at[turn], xu)
        arrived.wait_recv()
        arrived.wait_send()

    both_pairs = remote(pn, pn, ps.at[0], pr.at[0], xu)
    both_pairs.wait_recv()
    both_pairs.wait_send()
    for a, (up, low, shift) in enumerate(((FACE, 0, 0), (344, 144, 16))):
        wide = jnp.concatenate([pf[...], jnp.full((8, 384), -1000.0, F32)], axis=1)
        own = pltpu.roll(wide, up, 1)[a : a + 1, :]
        long = jnp.concatenate([pn[a], jnp.full((8, 256), -1000.0, F32)], axis=1)
        col = jnp.transpose(pltpu.roll(long, FACE + shift, 1))[:, a : a + 1]
        row = (iota((512, 640), 0) - shift).astype(F32)
        at_col = (iota((512, 640), 1) - low).astype(F32)
        px[a] = jnp.where((own == row) | (col == at_col), 1.0, 0.0).astype(BF16)

    def sent_x_rows(matrix, result):
        result[0:400, :] = dot(px[0, 0:400, :], matrix[0:640, :]).astype(BF16)

    def sent_y_rows(matrix, result):
        result[400:800, :] = dot(px[1, 16:416, :], matrix[256:896, :]).astype(BF16)

    def put(x, dst):
        high, low = halves(x)
        dst[:, 0:128] = high
        dst[:, 128:256] = low

    def joined(both):
        return both[:, 0:128] + both[:, 128:256]

    def product(matrix, chunks, result):
        def chunk(i):
            rows = pl.ds(pl.multiple_of(i * 400, 400), 400)
            result[rows, :] = joined(dot(matrix[rows, :], yb[...]))

        loop(0, chunks, chunk)

    def field(u, arrived, scale):
        return jnp.concatenate(
            [
                scale * (u[0:SHARED, :] - arrived[...]),
                jnp.zeros((FACE, LOADS), F32),
                (scale * ACTIVE_Z) * u[SHARED + FACE : ORDER, :],
            ],
            axis=0,
        )

    def total(a, b):
        return jnp.sum(a * b, axis=0, keepdims=True)

    def extras(*rows, size=8):
        sub = iota((size, 128), 0)
        tile = jnp.zeros((size, 128), F32)
        for i, row in enumerate(rows):
            tile = jnp.where(sub == i, row, tile)
        return tile

    def send_faces(src, dst, turn):
        for f in range(4):
            face_copy(src, dst, turn, f).start()

    def wait_faces(dst, turn):
        whole = remote(dst, dst, xs.at[turn], xr.at[turn], xu)
        whole.wait_recv()
        whole.wait_send()

    fetch[4].wait()
    sent_x_rows(sm, ss)

    half = remote(rx0.at[0:400], rx0.at[0:400], xs.at[0], xr.at[0], xu)
    half.wait_recv()
    half.wait_send()
    zeros = jnp.zeros((FACE, LOADS), F32)
    y0[...] = 0.5 * jnp.concatenate(
        [-rx0[0:FACE, :], rv[0], -rx0[2 * FACE : 3 * FACE, :], rv[1], zeros, ACTIVE_Z * rv[2]], axis=0
    )
    put(y0[...], yb)
    product(sm, 3, t0)
    start_energy = total(y0[...], t0[...])

    quarters = remote(phn.at[:, :, 0:384], phn.at[:, :, 0:384], fs.at[0], fr.at[0], xu)
    quarters.wait_recv()
    quarters.wait_send()
    at_lane = iota((24, 896), 1)
    blocks = []
    for blk in range(4):
        keep = (at_lane >= FACE * blk) & (at_lane < FACE * (blk + 1))
        blocks.append(jnp.where(keep, -phn[blk], 0.0))
    along_x = jnp.concatenate(blocks[0:2], axis=0)[:, 0:512].astype(BF16)
    along_y = jnp.concatenate(blocks[2:4], axis=0)[:, 384:896].astype(BF16)
    pef[24:72, 0:640] = dot(along_x, px[0])
    pef[72:120, 256:896] = dot(along_y, px[1])
    pe[...] = pef[...].astype(BF16)

    def corner_loads(t, result):
        put(t[...], tb)
        result[...] = 0.5 * joined(dot(pe[...], tb[...]))

    fetch[5].wait()
    corner_loads(t0, cl0)

    def coarse(turn, loads, tile, during_a, during_b, during_c, during_d):
        g = 4 * turn
        clt[...] = jnp.transpose(jnp.concatenate([loads, tile], axis=0))
        started(
            p, ring, lambda q: clt.at[pl.ds(pl.multiple_of(8 * q, 8), 8)], ra.at[turn], gs.at[0], gr.at[g]
        )
        ra[turn, p] = clt[pl.ds(pl.multiple_of(8 * p, 8), 8), :]
        during_a()
        ended(ra.at[turn], gs.at[0], gr.at[g])
        got = jnp.concatenate([ra[turn, i] for i in range(16)], axis=1)
        both = dot(stacked(got), at[...])
        mb[...] = both[0:8] + both[8:16]
        started(h, plane, lambda q: mb, rb.at[turn], gs.at[1], gr.at[g + 1])
        rb[turn, h] = mb[...]
        during_b()
        ended(rb.at[turn], gs.at[1], gr.at[g + 1])
        pieces, sums = [], jnp.zeros((8, 128), F32)
        for i in range(16):
            here, before, after = rb[turn, i], rb[turn, (i + 15) % 16], rb[turn, (i + 1) % 16]
            sums = sums + here[:, 0:128]
            part = jnp.where(lane < 96, here[:, 0:128] + before[:, 128:256], 0.0)
            part = part + jnp.where((lane >= 48) & (lane < 72), pltpu.roll(after[:, 0:128], 80, 1), 0.0)
            part = part + jnp.where((lane >= 72) & (lane < 96), pltpu.roll(after[:, 128:256], 104, 1), 0.0)
            pieces.append(part)
        four = lax.dot_general(
            stacked(jnp.concatenate(pieces, axis=1)), cp[...], NT, preferred_element_type=F32
        )
        sb[...] = joined(four[0:8]) + joined(four[8:16])
        started(h, plane, lambda q: sb, rc.at[turn], gs.at[0], gr.at[g + 2])
        rc[turn, h] = sb[...]
        during_c()
        ended(rc.at[turn], gs.at[0], gr.at[g + 2])
        got = jnp.concatenate([rc[turn, i] for i in range(16)], axis=1)
        both = dot(stacked(got), ohp[...])
        picked = both[0:8] + both[8:16]
        for q in range(16):
            first, by = divmod(24 * (q // 2), 128)
            at_tile = 384 * (q % 2) + 128 * first
            one = picked[:, at_tile : at_tile + 128]
            if by:
                two = picked[:, at_tile + 128 : at_tile + 256]
                one = jnp.where(lane < 128 - by, pltpu.roll(one, 128 - by, 1), pltpu.roll(two, 128 - by, 1))
            pb[q] = jnp.where(lane < 120, one, sums)
        started(p, ring, lambda q: pb.at[q], rd.at[turn], gs.at[1], gr.at[g + 3])
        rd[turn, p] = pb[p]
        during_d()
        ended(rd.at[turn], gs.at[1], gr.at[g + 3])
        solved = jnp.transpose(rd[turn].reshape(128, 128))
        high, low = halves(solved)
        corners = joined(dot(place, jnp.concatenate([high, low], axis=1)))
        return solved[120:128, :], corners

    def a0():
        rows_in(4, 0)
        below, above = 2 * ((gx + 6) & 7) + core, 2 * ((gx + 2) & 7) + core
        rows_to(below, xu, 1).start()
        rows_to(above, xd, 1).start()
        rows_to(below, device((gx + 2) & 7, gy), 1).start()
        sent_y_rows(sm, ss)
        product(ss, 2, ts)
        send_faces(ts, rx1, 1)
        ended(idr, ns.at[0], nr.at[0])
        idm[...] = sum([idr[i] for i in range(1, 16)], idr[0])
        started(h, plane, lambda q: idm, ids, ns.at[1], nr.at[1])
        ids[h] = idm[...]
        rows_in(3, 1)
        for k in range(1, 8):
            rows_to(2 * ((gx + k) & 7) + core, other, 2).start()
        fetch[6].wait()
        sent_x_rows(km, ks)

    def b0():
        rows_in(8, 2)
        for slot in range(16):
            for k in range(12):
                call[slot, 0:6, 128 * k : 128 * k + 128] = packed[slot, 6 * k : 6 * k + 6, :]
        high, low = halves(call[...].reshape(128, 1536))
        c256[0:128, :] = high
        c256[128:256, :] = low
        ended(ids, ns.at[1], nr.at[1])
        row = iota((1536, 256), 0)
        lanes = iota((1, 128), 1)

        def columns(j):
            pair_ids = [jnp.where(lanes < 96, ids[2 * j + s][0:1, :], -1.0) for s in range(2)]
            wanted = jnp.concatenate(pair_ids, axis=1).astype(jnp.int32)
            pick = (row == wanted).astype(F32).astype(BF16)
            cp[:, pl.ds(pl.multiple_of(j * 256, 256), 256)] = dot(c256[...], pick).astype(BF16)

        loop(0, 8, columns)

    def direction(t, arrived, w, turn, result):
        wait_faces(arrived, turn)
        w[...] = field(t, arrived, 0.5)
        put(w[...], yb)
        product(ks, 2, ts)
        send_faces(ts, result, turn + 1)
        return joined(dot(ph[...], yb[...]))

    kept = {}

    def c0():
        sent_y_rows(km, ks)
        kept["w0"] = direction(t0, rx1, w0, 1, rx2)
        nearby = jnp.concatenate([ids[(h + 15) & 15], ids[h], ids[(h + 1) & 15]], axis=1)
        fetch[7].wait()
        found = dot(stacked(nearby), ot[...])
        wanted = (found[0:1] + found[8:9]).astype(jnp.int32)

        def picks(j):
            rr = iota((128, 768), 0)
            own = 192 * (rr >> 4) + 12 * j + 6 * ((rr >> 3) & 1) + (rr & 7)
            own = jnp.where((rr & 7) < 6, own, -2)
            ohp[pl.ds(pl.multiple_of(j * 128, 128), 128), :] = (own == wanted).astype(F32).astype(BF16)

        loop(0, 16, picks)
        pet[...] = jnp.transpose(jnp.concatenate([pef[...], jnp.zeros((8, ORDER), F32)], axis=0)).astype(BF16)

        def chunk(i):
            rows = pl.ds(pl.multiple_of(i * 400, 400), 400)
            tp[rows, :] = dot(sm[rows, :], pet[...])

        loop(0, 3, chunk)

    def operator():
        put(tp[...], tb)
        through = 0.25 * joined(dot(pe[...], tb[...]))
        through = jnp.concatenate([through, jnp.zeros((8, 128), F32)], axis=0)
        high, low = halves(through)
        big[:, 0:128] = high
        big[:, 128:256] = low

    def second(d, arrived, turn, result):
        wait_faces(arrived, turn)
        yp[...] = field(d, arrived, 0.5)
        put(yp[...], yb)
        product(sm, 3, tp)
        corner_loads(tp, result)

    def coupled(corners):
        high, low = halves(corners)
        wide = jnp.concatenate([high, low], axis=1)
        return joined(dot(big[...], jnp.concatenate([wide, wide], axis=0)))[0:120]

    def d_first():
        product(km, 3, d0)
        operator()
        second(d0, rx2, 2, clm)
        kept["c00"] = total(w0[...], d0[...])
        kept["k1"] = total(t0[...], yp[...])
        kept["k2"] = total(yp[...], tp[...])

    sums, g0 = coarse(0, cl0[...], extras(start_energy), a0, b0, c0, d_first)
    start_energy = sums[0:1, :]
    g0x = g0[0:120]
    cl1[...] = clm[...] + coupled(g0)
    c00 = kept["c00"] + total(kept["w0"], g0[0:24])
    k1 = kept["k1"] + total(cl0[...], g0x)
    k2 = kept["k2"] + total(clm[...] + cl1[...], g0x)

    def a1():
        high, low = halves(0.5 * g0)
        yq[...] = yp[...] + joined(dot(pet[...], jnp.concatenate([high, low], axis=1)))
        put(yq[...], yb)
        product(ss, 2, ts)
        send_faces(ts, rx3, 3)
        product(sm, 3, tq)

    def b1():
        kept["wm"] = direction(tq, rx3, wm, 3, rx4)
        product(km, 3, dm)
        kept["c01"] = total(w0[...], dm[...])
        kept["c10"] = total(wm[...], d0[...]) + total(kept["wm"], g0[0:24])
        kept["c11"] = total(wm[...], dm[...])

    def c1():
        second(dm, rx4, 4, clm)
        kept["m1"] = total(t0[...], yp[...])
        kept["m2"] = total(tq[...], yp[...])
        kept["m3"] = total(yp[...], tp[...])

    sums, gm = coarse(1, cl1[...], extras(c00, k1, k2), a1, b1, c1, lambda: None)
    gmx = gm[0:120]
    alpha = start_energy / sums[0:1, :]
    energy = start_energy - 2.0 * alpha * sums[1:2, :] + alpha * alpha * sums[2:3, :]
    ratio = 1.0 + energy / start_energy
    c01 = kept["c01"] + kept["c10"] + total(kept["w0"], gm[0:24])
    c11 = kept["c11"] + total(kept["wm"], gm[0:24])
    m1 = kept["m1"] + total(cl0[...], gmx)
    m2 = kept["m2"] + total(cl1[...], gmx)
    m3 = kept["m3"] + total(2.0 * clm[...] + coupled(gm), gmx)
    curvature = ratio * ratio * c00 - ratio * alpha * c01 + alpha * alpha * c11
    cross = ratio * (k1 - alpha * k2) - alpha * (m1 - alpha * m2)
    square = ratio * ratio * k2 - 2.0 * ratio * alpha * m2 + alpha * alpha * m3
    fb0[...] = extras(curvature, cross, square, size=4)
    started(p, ring, lambda q: fb0, fb1, gs.at[0], gr.at[8])
    fb1[p] = fb0[...]
    ended(fb1, gs.at[0], gr.at[8])
    fb2[...] = sum([fb1[i] for i in range(1, 16)], fb1[0])
    started(h, plane, lambda q: fb2, fb3, gs.at[1], gr.at[9])
    fb3[h] = fb2[...]
    ended(fb3, gs.at[1], gr.at[9])
    sums = sum([fb3[i] for i in range(1, 16)], fb3[0])
    step = energy / sums[0:1, :]
    final = energy - 2.0 * step * sums[1:2, :] + step * step * sums[2:3, :]
    red[...] = final / start_energy
    for a in range(3):
        rows = slice(FACE * (2 * a + 1), FACE * (2 * a + 2))
        out[a] = (alpha + step * ratio) * w0[rows, :] - (step * alpha) * wm[rows, :]


def hand_over(a, b, out, red):
    out[...] = a[...]
    red[...] = b[...]


def local(rhs, stiff, schur, phi, coarse, inc, pair):
    table, order = jnp.asarray(assembly_table(), BF16), jnp.asarray(order_table(), BF16)
    v = pltpu.VMEM
    wide, sent = v((ORDER, LOADS), F32), v((SHARED, LOADS), F32)
    dma = pltpu.SemaphoreType.DMA
    tile, group = v((8, 128), F32), v((16, 8, 128), F32)
    scratch = [
        v((3, FACE, LOADS), F32), v((ORDER, ORDER), BF16), v((ORDER, ORDER), BF16),
        v((SHARED, ORDER), BF16), v((SHARED, ORDER), BF16),
        v((24, ORDER), BF16), v((24, ORDER), F32), v((4, 24, 896), F32),
        v((6, 1536), F32), v((16, 72, 128), F32), v((16, 8, 1536), F32), v((3, 1, FACE), jnp.int32), v((8, 256), F32), v((2, 8, 256), F32),
        v((2048, 256), BF16), v((384, 768), BF16),
        v((ORDER, 256), BF16), v((ORDER, 256), BF16),
        sent, sent, sent, sent, sent, sent, sent,
        wide, wide, wide, wide, wide, wide, wide, wide, wide, wide,
        v((2, 512, 640), BF16), v((120, ORDER), F32), v((120, ORDER), BF16), v((ORDER, 128), BF16),
        v((128, 256), BF16), v((128, 128), F32), v((120, 128), F32), v((120, 128), F32), v((120, 128), F32),
        v((2, 16, 8, 128), F32), v((8, 256), F32), v((2, 16, 8, 256), F32),
        tile, v((2, 16, 8, 128), F32), group, v((2, 16, 8, 128), F32),
        v((256, 2048), BF16), v((256, 1536), BF16), v((2048, 768), BF16),
        tile, group, tile, group,
        v((4, 128), F32), v((16, 4, 128), F32), v((4, 128), F32), v((16, 4, 128), F32),
        dma((8,)), dma((5,)), dma((5,)), dma((1,)), dma((1,)), dma((1,)), dma((1,)),
        dma((2,)), dma((2,)), dma((3,)), dma((3,)), dma((2,)), dma((10,)),
    ]
    any_space = pl.BlockSpec(memory_space=pl.ANY)
    in_vmem = pl.BlockSpec(memory_space=pltpu.VMEM)
    shapes = (jax.ShapeDtypeStruct((3, FACE, LOADS), F32), jax.ShapeDtypeStruct((1, LOADS), F32))
    result, reduction = pl.pallas_call(
        kernel,
        out_shape=shapes,
        in_specs=[any_space] * 5 + [pl.BlockSpec(memory_space=pltpu.SMEM)] + [any_space] * 3,
        out_specs=(in_vmem, in_vmem),
        scratch_shapes=scratch,
        compiler_params=pltpu.CompilerParams(
            collective_id=0, has_side_effects=True, vmem_limit_bytes=60 * 1024 * 1024
        ),
        name="domain_decomposition",
    )(
        rhs[0, 0, 0], stiff[0, 0, 0], schur[0, 0, 0], phi[0, 0, 0], coarse, inc[0, 0, 0],
        pair.reshape(3, 1, FACE), table, order,
    )
    result, reduction = pl.pallas_call(
        hand_over, out_shape=shapes, in_specs=[in_vmem] * 2, out_specs=(in_vmem, in_vmem), name="hand_over"
    )(result, reduction)
    return result[None, None, None], reduction[0]


def solution(mesh):
    four = P("gx", "gy", None, None)
    five = P("gx", "gy", None, None, None)
    six = P("gx", "gy", None, None, None, None)
    return jax.shard_map(
        local,
        mesh=mesh,
        in_specs=(six, five, five, five, P(("gx", "gy"), None), four, five),
        out_specs=(six, P()),
        check_vma=False,
    )
```

```python
import jax
import jax.numpy as jnp
import numpy as np
from jax import lax
from jax.experimental import pallas as pl
from jax.experimental.pallas import tpu as pltpu
from jax.sharding import PartitionSpec as P

F32, BF16 = jnp.float32, jnp.bfloat16
MESH = pl.DeviceIdType.MESH
HIGHEST = lax.Precision.HIGHEST
FACE, ORDER, LOADS = 200, 1200, 128
SHARED = 4 * FACE
ACTIVE_Z = 0.0
NT = (((1,), (1,)), ((), ()))


def assembly_table():
    table = np.zeros((16, 128, 256), np.float32)
    steps = ((0, 0), (1, 0), (-1, 0), (0, 1), (0, -1))
    for p in range(16):
        x, core = p // 2, p % 2
        for block, (ox, oy) in enumerate(steps):
            for c in range(8):
                gx = (x + ox + c % 2) % 8
                y = core + oy + (c // 2) % 2
                z = c // 4
                for i in range(3):
                    if y == -1:
                        m = 128 * z + 96 + gx * 3 + i
                    else:
                        m = 128 * (y // 2) + (y % 2) * 48 + z * 24 + gx * 3 + i
                    table[p, block * 24 + 3 * c + i, m] = 1.0
        for e in range(8):
            table[p, 120 + e, 120 + e] = 1.0
    return table.reshape(2048, 256)


def order_table():
    table = np.zeros((384, 768), np.float32)
    for core in range(2):
        for slot in range(11):
            for y in range(4):
                for z in range(2):
                    for i in range(3):
                        chip, half = divmod(core + 1 + y, 2)
                        lane = chip * 128 + half * 48 + z * 24 + (slot - 1) % 8 * 3 + i
                        table[lane, 384 * core + slot * 24 + y * 6 + z * 3 + i] = 1.0
    return table


def loop(low, high, step):
    def body(k, carry):
        step(k)
        return carry

    lax.fori_loop(low, high, body, 0)


def halves(x):
    high = x.astype(BF16)
    return high, (x - high.astype(F32)).astype(BF16)


def stacked(x):
    high = x.astype(BF16).astype(F32)
    return jnp.concatenate([high, x - high], axis=0).astype(BF16)


def iota(shape, dim):
    return lax.broadcasted_iota(jnp.int32, shape, dim)


def dot(a, b):
    return jnp.dot(a, b, preferred_element_type=F32)


def kernel(
    rhs, stiff, schur, phi, coarse, inc, pair, table, order,
    out, red,
    rv, sm, km, ss, ks, ph, phf, phn, cin, packed, call, pin, pf, pn, at, ot,
    yb, tb, ts, rx0, rx1, rx2, rx3, rx4, snd,
    y0, t0, w0, d0, yp, yq, tq, wm, dm, tp,
    px, pef, pe, pet, big, clt, cl0, cl1, clm,
    ra, mb, rb, sb, rc, pb, rd, cp, c256, ohp, idt, idr, idm, ids, fb0, fb1, fb2, fb3,
    hsem, xs, xr, ps, pr, fs, fr, ns, nr, cs, cr, gs, gr,
):
    gx, gy = lax.axis_index("gx"), lax.axis_index("gy")
    h, core = gy // 2, gy % 2
    p = gx * 2 + core

    def device(x, y):
        return {"gx": x, "gy": y}

    def ring(q):
        return device(q >> 1, 2 * h + (q & 1))

    def plane(other):
        return device(gx, 2 * other + core)

    xu, xd = device((gx + 1) & 7, gy), device((gx + 7) & 7, gy)
    yu, yd = device(gx, (gy + 1) & 31), device(gx, (gy + 31) & 31)

    def remote(src, dst, send, recv, target):
        return pltpu.make_async_remote_copy(
            src_ref=src, dst_ref=dst, send_sem=send, recv_sem=recv, device_id=target, device_id_type=MESH
        )

    loads = [(rhs, rv), (pair, pin), (phi, ph), (coarse, cin), (schur, sm), (table, at), (stiff, km), (order, ot)]
    fetch = [pltpu.make_async_copy(a, b, hsem.at[i]) for i, (a, b) in enumerate(loads)]
    for f in fetch:
        f.start()

    barrier = pltpu.get_barrier_semaphore()

    def greet(target):
        pl.semaphore_signal(barrier, inc=1, device_id=target, device_id_type=MESH)

    loop(1, 16, lambda k: greet(ring((p + k) & 15)))
    loop(1, 16, lambda k: greet(plane((h + k) & 15)))
    greet(yu)
    greet(yd)

    fetch[0].wait()
    fetch[1].wait()
    pf[...] = jnp.full((8, 256), -1000.0, F32)
    for a in range(2):
        pf[a : a + 1, 0:FACE] = pin[a].astype(F32)
    down = iota((FACE, FACE), 0).astype(F32)
    for a in range(2):
        onto = (pf[a : a + 1, 0:FACE] == down).astype(F32)
        snd[400 * a : 400 * a + FACE, :] = jnp.dot(onto, rv[a], precision=HIGHEST, preferred_element_type=F32)

    pl.semaphore_wait(barrier, 32)

    def face_copy(src, dst, turn, face):
        rows = pl.ds(FACE * face, FACE)
        return remote(src.at[rows], dst.at[rows], xs.at[turn], xr.at[turn], (xu, xd, yu, yd)[face])

    for a in range(2):
        remote(pf, pn.at[a], ps.at[0], pr.at[0], (xu, yu)[a]).start()
    for f in (0, 2):
        face_copy(snd, rx0, 0, f).start()
    lane = iota((8, 128), 1)
    mine = jnp.zeros((8, 128), F32)
    for z in range(2):
        base = core * 48 + z * 24 + gx * 3
        node = jnp.full((8, 128), inc[4 * z], jnp.int32)
        mine = jnp.where((lane >= base) & (lane < base + 3), (3 * node + (lane - base)).astype(F32), mine)
    idt[...] = mine
    idr[p] = mine

    fetch[2].wait()
    phf[...] = ph[...].astype(F32)
    fetch[3].wait()
    for k in range(12):
        packed[p, 6 * k : 6 * k + 6, :] = cin[:, 128 * k : 128 * k + 128]
    call[...] = jnp.zeros((16, 8, 1536), F32)

    full = iota((24, ORDER), 1)
    zone = jnp.where(full < SHARED, 1.0, jnp.where(full < SHARED + FACE, 0.0, ACTIVE_Z))
    pef[...] = jnp.zeros((120, ORDER), F32)
    pef[0:24, :] = phf[...] * zone
    r, m = iota((128, 128), 0), iota((128, 128), 1)
    block = (r * 683) >> 14
    e = r - 24 * block
    c = (e * 11) >> 5
    over = 1 + jnp.where(block == 1, 1, 0) - jnp.where(block == 2, 1, 0) + (c & 1)
    up = 1 + jnp.where(block == 3, 1, 0) - jnp.where(block == 4, 1, 0) + ((c >> 1) & 1)
    to = over * 24 + up * 6 + (c >> 2) * 3 + (e - 3 * c)
    place = ((to == m) & (r < 120)).astype(F32).astype(BF16)

    windows = ((0, 384), (128, 512), (384, 768), (512, 896))
    for blk, target in enumerate((xd, xu, yd, yu)):
        low, high = windows[blk]
        remote(phf.at[:, low:high], phn.at[blk, :, low:high], fs.at[0], fr.at[0], target).start()

    def far(step, size):
        return min(step, size - step)

    ring_steps = sorted(((dx, dc) for dx in range(8) for dc in (1, 0)), key=lambda d: -far(d[0], 8))
    ring_others = [2 * ((gx + dx) & 7) + ((core + dc) & 1) for dx, dc in ring_steps if dx or dc]
    plane_steps = sorted(
        ((dy, dx) for dy in range(4) for dx in range(4)), key=lambda d: -far(d[0], 4) - far(d[1], 4)
    )
    plane_others = [4 * (((h >> 2) + dy) & 3) + ((h + dx) & 3) for dy, dx in plane_steps if dy or dx]

    def started(me, where, src, dst, send, recv):
        for q in ring_others if where is ring else plane_others:
            remote(src(q), dst.at[me], send, recv, where(q)).start()

    def ended(dst, send, recv):
        all_blocks = remote(dst.at[0:15], dst.at[0:15], send, recv, xu)
        all_blocks.wait_recv()
        all_blocks.wait_send()

    other = device(gx, 2 * h + 1 - core)

    def rows_to(slot, target, turn):
        return remote(packed.at[slot], packed.at[slot], cs.at[turn], cr.at[turn], target)

    for k in (1, 7, 2, 6):
        rows_to(p, device((gx + k) & 7, gy), 0).start()
    rows_to(p, other, 2).start()
    started(p, ring, lambda q: idt, idr, ns.at[0], nr.at[0])

    def rows_in(count, turn):
        some = packed.at[0:count]
        arrived = remote(some, some, cs.at[turn], cr.at[turn], xu)
        arrived.wait_recv()
        arrived.wait_send()

    both_pairs = remote(pn, pn, ps.at[0], pr.at[0], xu)
    both_pairs.wait_recv()
    both_pairs.wait_send()
    for a, (up, low, shift) in enumerate(((FACE, 0, 0), (344, 144, 16))):
        wide = jnp.concatenate([pf[...], jnp.full((8, 384), -1000.0, F32)], axis=1)
        own = pltpu.roll(wide, up, 1)[a : a + 1, :]
        long = jnp.concatenate([pn[a], jnp.full((8, 256), -1000.0, F32)], axis=1)
        col = jnp.transpose(pltpu.roll(long, FACE + shift, 1))[:, a : a + 1]
        row = (iota((512, 640), 0) - shift).astype(F32)
        at_col = (iota((512, 640), 1) - low).astype(F32)
        px[a] = jnp.where((own == row) | (col == at_col), 1.0, 0.0).astype(BF16)

    def sent_x_rows(matrix, result):
        result[0:400, :] = dot(px[0, 0:400, :], matrix[0:640, :]).astype(BF16)

    def sent_y_rows(matrix, result):
        result[400:800, :] = dot(px[1, 16:416, :], matrix[256:896, :]).astype(BF16)

    def put(x, dst):
        high, low = halves(x)
        dst[:, 0:128] = high
        dst[:, 128:256] = low

    def joined(both):
        return both[:, 0:128] + both[:, 128:256]

    def product(matrix, chunks, result):
        def chunk(i):
            rows = pl.ds(pl.multiple_of(i * 400, 400), 400)
            result[rows, :] = joined(dot(matrix[rows, :], yb[...]))

        loop(0, chunks, chunk)

    def field(u, arrived, scale):
        return jnp.concatenate(
            [
                scale * (u[0:SHARED, :] - arrived[...]),
                jnp.zeros((FACE, LOADS), F32),
                (scale * ACTIVE_Z) * u[SHARED + FACE : ORDER, :],
            ],
            axis=0,
        )

    def total(a, b):
        return jnp.sum(a * b, axis=0, keepdims=True)

    def extras(*rows, size=8):
        sub = iota((size, 128), 0)
        tile = jnp.zeros((size, 128), F32)
        for i, row in enumerate(rows):
            tile = jnp.where(sub == i, row, tile)
        return tile

    def send_faces(src, dst, turn):
        for f in range(4):
            face_copy(src, dst, turn, f).start()

    def wait_faces(dst, turn):
        whole = remote(dst, dst, xs.at[turn], xr.at[turn], xu)
        whole.wait_recv()
        whole.wait_send()

    fetch[4].wait()
    sent_x_rows(sm, ss)

    half = remote(rx0.at[0:400], rx0.at[0:400], xs.at[0], xr.at[0], xu)
    half.wait_recv()
    half.wait_send()
    zeros = jnp.zeros((FACE, LOADS), F32)
    y0[...] = 0.5 * jnp.concatenate(
        [-rx0[0:FACE, :], rv[0], -rx0[2 * FACE : 3 * FACE, :], rv[1], zeros, ACTIVE_Z * rv[2]], axis=0
    )
    put(y0[...], yb)
    product(sm, 3, t0)
    start_energy = total(y0[...], t0[...])

    quarters = remote(phn.at[:, :, 0:384], phn.at[:, :, 0:384], fs.at[0], fr.at[0], xu)
    quarters.wait_recv()
    quarters.wait_send()
    at_lane = iota((24, 896), 1)
    blocks = []
    for blk in range(4):
        keep = (at_lane >= FACE * blk) & (at_lane < FACE * (blk + 1))
        blocks.append(jnp.where(keep, -phn[blk], 0.0))
    along_x = jnp.concatenate(blocks[0:2], axis=0)[:, 0:512].astype(BF16)
    along_y = jnp.concatenate(blocks[2:4], axis=0)[:, 384:896].astype(BF16)
    pef[24:72, 0:640] = dot(along_x, px[0])
    pef[72:120, 256:896] = dot(along_y, px[1])
    pe[...] = pef[...].astype(BF16)

    def corner_loads(t, result):
        put(t[...], tb)
        result[...] = 0.5 * joined(dot(pe[...], tb[...]))

    fetch[5].wait()
    corner_loads(t0, cl0)

    def coarse(turn, loads, tile, during_a, during_b, during_c, during_d):
        g = 4 * turn
        clt[...] = jnp.transpose(jnp.concatenate([loads, tile], axis=0))
        started(
            p, ring, lambda q: clt.at[pl.ds(pl.multiple_of(8 * q, 8), 8)], ra.at[turn], gs.at[0], gr.at[g]
        )
        ra[turn, p] = clt[pl.ds(pl.multiple_of(8 * p, 8), 8), :]
        during_a()
        ended(ra.at[turn], gs.at[0], gr.at[g])
        got = jnp.concatenate([ra[turn, i] for i in range(16)], axis=1)
        both = dot(stacked(got), at[...])
        mb[...] = both[0:8] + both[8:16]
        started(h, plane, lambda q: mb, rb.at[turn], gs.at[1], gr.at[g + 1])
        rb[turn, h] = mb[...]
        during_b()
        ended(rb.at[turn], gs.at[1], gr.at[g + 1])
        pieces, sums = [], jnp.zeros((8, 128), F32)
        for i in range(16):
            here, before, after = rb[turn, i], rb[turn, (i + 15) % 16], rb[turn, (i + 1) % 16]
            sums = sums + here[:, 0:128]
            part = jnp.where(lane < 96, here[:, 0:128] + before[:, 128:256], 0.0)
            part = part + jnp.where((lane >= 48) & (lane < 72), pltpu.roll(after[:, 0:128], 80, 1), 0.0)
            part = part + jnp.where((lane >= 72) & (lane < 96), pltpu.roll(after[:, 128:256], 104, 1), 0.0)
            pieces.append(part)
        four = lax.dot_general(
            stacked(jnp.concatenate(pieces, axis=1)), cp[...], NT, preferred_element_type=F32
        )
        sb[...] = joined(four[0:8]) + joined(four[8:16])
        started(h, plane, lambda q: sb, rc.at[turn], gs.at[0], gr.at[g + 2])
        rc[turn, h] = sb[...]
        during_c()
        ended(rc.at[turn], gs.at[0], gr.at[g + 2])
        got = jnp.concatenate([rc[turn, i] for i in range(16)], axis=1)
        both = dot(stacked(got), ohp[...])
        picked = both[0:8] + both[8:16]
        for q in range(16):
            first, by = divmod(24 * (q // 2), 128)
            at_tile = 384 * (q % 2) + 128 * first
            one = picked[:, at_tile : at_tile + 128]
            if by:
                two = picked[:, at_tile + 128 : at_tile + 256]
                one = jnp.where(lane < 128 - by, pltpu.roll(one, 128 - by, 1), pltpu.roll(two, 128 - by, 1))
            pb[q] = jnp.where(lane < 120, one, sums)
        started(p, ring, lambda q: pb.at[q], rd.at[turn], gs.at[1], gr.at[g + 3])
        rd[turn, p] = pb[p]
        during_d()
        ended(rd.at[turn], gs.at[1], gr.at[g + 3])
        solved = jnp.transpose(rd[turn].reshape(128, 128))
        high, low = halves(solved)
        corners = joined(dot(place, jnp.concatenate([high, low], axis=1)))
        return solved[120:128, :], corners

    def a0():
        rows_in(4, 0)
        below, above = 2 * ((gx + 6) & 7) + core, 2 * ((gx + 2) & 7) + core
        rows_to(below, xu, 1).start()
        rows_to(above, xd, 1).start()
        rows_to(below, device((gx + 2) & 7, gy), 1).start()
        sent_y_rows(sm, ss)
        product(ss, 2, ts)
        send_faces(ts, rx1, 1)
        ended(idr, ns.at[0], nr.at[0])
        idm[...] = sum([idr[i] for i in range(1, 16)], idr[0])
        started(h, plane, lambda q: idm, ids, ns.at[1], nr.at[1])
        ids[h] = idm[...]
        fetch[6].wait()
        sent_x_rows(km, ks)
        sent_y_rows(km, ks)

    def b0():
        rows_in(3, 1)
        for k in range(1, 8):
            rows_to(2 * ((gx + k) & 7) + core, other, 2).start()
        rows_in(8, 2)
        for slot in range(16):
            for k in range(12):
                call[slot, 0:6, 128 * k : 128 * k + 128] = packed[slot, 6 * k : 6 * k + 6, :]
        high, low = halves(call[...].reshape(128, 1536))
        c256[0:128, :] = high
        c256[128:256, :] = low
        ended(ids, ns.at[1], nr.at[1])
        row = iota((1536, 256), 0)
        lanes = iota((1, 128), 1)

        def columns(j):
            pair_ids = [jnp.where(lanes < 96, ids[2 * j + s][0:1, :], -1.0) for s in range(2)]
            wanted = jnp.concatenate(pair_ids, axis=1).astype(jnp.int32)
            pick = (row == wanted).astype(F32).astype(BF16)
            cp[:, pl.ds(pl.multiple_of(j * 256, 256), 256)] = dot(c256[...], pick).astype(BF16)

        loop(0, 8, columns)

    def direction(t, arrived, w, turn, result):
        wait_faces(arrived, turn)
        w[...] = field(t, arrived, 0.5)
        put(w[...], yb)
        product(ks, 2, ts)
        send_faces(ts, result, turn + 1)
        return joined(dot(ph[...], yb[...]))

    kept = {}

    def c0():
        kept["w0"] = direction(t0, rx1, w0, 1, rx2)
        nearby = jnp.concatenate([ids[(h + 15) & 15], ids[h], ids[(h + 1) & 15]], axis=1)
        fetch[7].wait()
        found = dot(stacked(nearby), ot[...])
        wanted = (found[0:1] + found[8:9]).astype(jnp.int32)

        def picks(j):
            rr = iota((128, 768), 0)
            own = 192 * (rr >> 4) + 12 * j + 6 * ((rr >> 3) & 1) + (rr & 7)
            own = jnp.where((rr & 7) < 6, own, -2)
            ohp[pl.ds(pl.multiple_of(j * 128, 128), 128), :] = (own == wanted).astype(F32).astype(BF16)

        loop(0, 16, picks)
        pet[...] = jnp.transpose(jnp.concatenate([pef[...], jnp.zeros((8, ORDER), F32)], axis=0)).astype(BF16)

        def chunk(i):
            rows = pl.ds(pl.multiple_of(i * 400, 400), 400)
            tp[rows, :] = dot(sm[rows, :], pet[...])

        loop(0, 3, chunk)

    def operator():
        put(tp[...], tb)
        through = 0.25 * joined(dot(pe[...], tb[...]))
        through = jnp.concatenate([through, jnp.zeros((8, 128), F32)], axis=0)
        high, low = halves(through)
        big[:, 0:128] = high
        big[:, 128:256] = low

    def second(d, arrived, turn, result):
        wait_faces(arrived, turn)
        yp[...] = field(d, arrived, 0.5)
        put(yp[...], yb)
        product(sm, 3, tp)
        corner_loads(tp, result)

    def coupled(corners):
        high, low = halves(corners)
        wide = jnp.concatenate([high, low], axis=1)
        return joined(dot(big[...], jnp.concatenate([wide, wide], axis=0)))[0:120]

    def d_first():
        product(km, 3, d0)
        operator()
        second(d0, rx2, 2, clm)
        kept["c00"] = total(w0[...], d0[...])
        kept["k1"] = total(t0[...], yp[...])
        kept["k2"] = total(yp[...], tp[...])

    sums, g0 = coarse(0, cl0[...], extras(start_energy), a0, b0, c0, d_first)
    start_energy = sums[0:1, :]
    g0x = g0[0:120]
    cl1[...] = clm[...] + coupled(g0)
    c00 = kept["c00"] + total(kept["w0"], g0[0:24])
    k1 = kept["k1"] + total(cl0[...], g0x)
    k2 = kept["k2"] + total(clm[...] + cl1[...], g0x)

    def a1():
        high, low = halves(0.5 * g0)
        yq[...] = yp[...] + joined(dot(pet[...], jnp.concatenate([high, low], axis=1)))
        put(yq[...], yb)
        product(ss, 2, ts)
        send_faces(ts, rx3, 3)
        product(sm, 3, tq)

    def b1():
        kept["wm"] = direction(tq, rx3, wm, 3, rx4)
        product(km, 3, dm)
        kept["c01"] = total(w0[...], dm[...])
        kept["c10"] = total(wm[...], d0[...]) + total(kept["wm"], g0[0:24])
        kept["c11"] = total(wm[...], dm[...])

    def c1():
        second(dm, rx4, 4, clm)
        kept["m1"] = total(t0[...], yp[...])
        kept["m2"] = total(tq[...], yp[...])
        kept["m3"] = total(yp[...], tp[...])

    sums, gm = coarse(1, cl1[...], extras(c00, k1, k2), a1, b1, c1, lambda: None)
    gmx = gm[0:120]
    alpha = start_energy / sums[0:1, :]
    energy = start_energy - 2.0 * alpha * sums[1:2, :] + alpha * alpha * sums[2:3, :]
    ratio = 1.0 + energy / start_energy
    c01 = kept["c01"] + kept["c10"] + total(kept["w0"], gm[0:24])
    c11 = kept["c11"] + total(kept["wm"], gm[0:24])
    m1 = kept["m1"] + total(cl0[...], gmx)
    m2 = kept["m2"] + total(cl1[...], gmx)
    m3 = kept["m3"] + total(2.0 * clm[...] + coupled(gm), gmx)
    curvature = ratio * ratio * c00 - ratio * alpha * c01 + alpha * alpha * c11
    cross = ratio * (k1 - alpha * k2) - alpha * (m1 - alpha * m2)
    square = ratio * ratio * k2 - 2.0 * ratio * alpha * m2 + alpha * alpha * m3
    fb0[...] = extras(curvature, cross, square, size=4)
    started(p, ring, lambda q: fb0, fb1, gs.at[0], gr.at[8])
    fb1[p] = fb0[...]
    ended(fb1, gs.at[0], gr.at[8])
    fb2[...] = sum([fb1[i] for i in range(1, 16)], fb1[0])
    started(h, plane, lambda q: fb2, fb3, gs.at[1], gr.at[9])
    fb3[h] = fb2[...]
    ended(fb3, gs.at[1], gr.at[9])
    sums = sum([fb3[i] for i in range(1, 16)], fb3[0])
    step = energy / sums[0:1, :]
    final = energy - 2.0 * step * sums[1:2, :] + step * step * sums[2:3, :]
    red[...] = final / start_energy
    for a in range(3):
        rows = slice(FACE * (2 * a + 1), FACE * (2 * a + 2))
        out[a] = (alpha + step * ratio) * w0[rows, :] - (step * alpha) * wm[rows, :]


def local(rhs, stiff, schur, phi, coarse, inc, pair):
    table, order = jnp.asarray(assembly_table(), BF16), jnp.asarray(order_table(), BF16)
    v = pltpu.VMEM
    wide, sent = v((ORDER, LOADS), F32), v((SHARED, LOADS), F32)
    dma = pltpu.SemaphoreType.DMA
    tile, group = v((8, 128), F32), v((16, 8, 128), F32)
    scratch = [
        v((3, FACE, LOADS), F32), v((ORDER, ORDER), BF16), v((ORDER, ORDER), BF16),
        v((SHARED, ORDER), BF16), v((SHARED, ORDER), BF16),
        v((24, ORDER), BF16), v((24, ORDER), F32), v((4, 24, 896), F32),
        v((6, 1536), F32), v((16, 72, 128), F32), v((16, 8, 1536), F32), v((3, 1, FACE), jnp.int32), v((8, 256), F32), v((2, 8, 256), F32),
        v((2048, 256), BF16), v((384, 768), BF16),
        v((ORDER, 256), BF16), v((ORDER, 256), BF16),
        sent, sent, sent, sent, sent, sent, sent,
        wide, wide, wide, wide, wide, wide, wide, wide, wide, wide,
        v((2, 512, 640), BF16), v((120, ORDER), F32), v((120, ORDER), BF16), v((ORDER, 128), BF16),
        v((128, 256), BF16), v((128, 128), F32), v((120, 128), F32), v((120, 128), F32), v((120, 128), F32),
        v((2, 16, 8, 128), F32), v((8, 256), F32), v((2, 16, 8, 256), F32),
        tile, v((2, 16, 8, 128), F32), group, v((2, 16, 8, 128), F32),
        v((256, 2048), BF16), v((256, 1536), BF16), v((2048, 768), BF16),
        tile, group, tile, group,
        v((4, 128), F32), v((16, 4, 128), F32), v((4, 128), F32), v((16, 4, 128), F32),
        dma((8,)), dma((5,)), dma((5,)), dma((1,)), dma((1,)), dma((1,)), dma((1,)),
        dma((2,)), dma((2,)), dma((3,)), dma((3,)), dma((2,)), dma((10,)),
    ]
    any_space = pl.BlockSpec(memory_space=pl.ANY)
    in_vmem = pl.BlockSpec(memory_space=pltpu.VMEM)
    result, reduction = pl.pallas_call(
        kernel,
        out_shape=(v((3, FACE, LOADS), F32), v((1, LOADS), F32)),
        in_specs=[any_space] * 5 + [pl.BlockSpec(memory_space=pltpu.SMEM)] + [any_space] * 3,
        out_specs=(in_vmem, in_vmem),
        scratch_shapes=scratch,
        compiler_params=pltpu.CompilerParams(
            collective_id=0, has_side_effects=True, vmem_limit_bytes=60 * 1024 * 1024
        ),
        name="domain_decomposition",
    )(
        rhs[0, 0, 0], stiff[0, 0, 0], schur[0, 0, 0], phi[0, 0, 0], coarse, inc[0, 0, 0],
        pair.reshape(3, 1, FACE), table, order,
    )
    return result[None, None, None], reduction[0]


def solution(mesh):
    four = P("gx", "gy", None, None)
    five = P("gx", "gy", None, None, None)
    six = P("gx", "gy", None, None, None, None)
    return jax.shard_map(
        local,
        mesh=mesh,
        in_specs=(six, five, five, five, P(("gx", "gy"), None), four, five),
        out_specs=(six, P()),
        check_vma=False,
    )
```

```python
import jax
import jax.numpy as jnp
import numpy as np
from jax import lax
from jax.experimental import pallas as pl
from jax.experimental.pallas import tpu as pltpu
from jax.sharding import PartitionSpec as P

F32, BF16 = jnp.float32, jnp.bfloat16
MESH = pl.DeviceIdType.MESH
HIGHEST = lax.Precision.HIGHEST
FACE, ORDER, LOADS = 200, 1200, 128
SHARED = 4 * FACE
ACTIVE_Z = 0.0
NT = (((1,), (1,)), ((), ()))


def assembly_table():
    table = np.zeros((16, 128, 256), np.float32)
    steps = ((0, 0), (1, 0), (-1, 0), (0, 1), (0, -1))
    for p in range(16):
        x, core = p // 2, p % 2
        for block, (ox, oy) in enumerate(steps):
            for c in range(8):
                gx = (x + ox + c % 2) % 8
                y = core + oy + (c // 2) % 2
                z = c // 4
                for i in range(3):
                    if y == -1:
                        m = 128 * z + 96 + gx * 3 + i
                    else:
                        m = 128 * (y // 2) + (y % 2) * 48 + z * 24 + gx * 3 + i
                    table[p, block * 24 + 3 * c + i, m] = 1.0
        for e in range(8):
            table[p, 120 + e, 120 + e] = 1.0
    return table.reshape(2048, 256)


def order_table():
    table = np.zeros((384, 768), np.float32)
    for core in range(2):
        for slot in range(11):
            for y in range(4):
                for z in range(2):
                    for i in range(3):
                        chip, half = divmod(core + 1 + y, 2)
                        lane = chip * 128 + half * 48 + z * 24 + (slot - 1) % 8 * 3 + i
                        table[lane, 384 * core + slot * 24 + y * 6 + z * 3 + i] = 1.0
    return table


def loop(low, high, step):
    def body(k, carry):
        step(k)
        return carry

    lax.fori_loop(low, high, body, 0)


def halves(x):
    high = x.astype(BF16)
    return high, (x - high.astype(F32)).astype(BF16)


def stacked(x):
    high = x.astype(BF16).astype(F32)
    return jnp.concatenate([high, x - high], axis=0).astype(BF16)


def iota(shape, dim):
    return lax.broadcasted_iota(jnp.int32, shape, dim)


def dot(a, b):
    return jnp.dot(a, b, preferred_element_type=F32)


def kernel(
    rhs, stiff, schur, phi, coarse, inc, pair, table, order,
    out, red,
    rv, sm, km, ss, ks, ph, phf, phn, cin, packed, call, pin, pf, pn, at, ot,
    yb, tb, ts, rx0, rx1, rx2, rx3, rx4, snd,
    y0, t0, w0, d0, yp, yq, tq, wm, dm, tp,
    px, pef, pe, pet, big, clt, cl0, cl1, clm,
    ra, mb, rb, sb, rc, pb, rd, cp, c256, ohp, idt, idr, idm, ids, fb0, fb1, fb2, fb3,
    hsem, xs, xr, ps, pr, fs, fr, ns, nr, cs, cr, gs, gr,
):
    gx, gy = lax.axis_index("gx"), lax.axis_index("gy")
    h, core = gy // 2, gy % 2
    p = gx * 2 + core

    def device(x, y):
        return {"gx": x, "gy": y}

    def ring(q):
        return device(q >> 1, 2 * h + (q & 1))

    def plane(other):
        return device(gx, 2 * other + core)

    xu, xd = device((gx + 1) & 7, gy), device((gx + 7) & 7, gy)
    yu, yd = device(gx, (gy + 1) & 31), device(gx, (gy + 31) & 31)

    def remote(src, dst, send, recv, target):
        return pltpu.make_async_remote_copy(
            src_ref=src, dst_ref=dst, send_sem=send, recv_sem=recv, device_id=target, device_id_type=MESH
        )

    loads = [(rhs, rv), (pair, pin), (phi, ph), (coarse, cin), (schur, sm), (table, at), (stiff, km), (order, ot)]
    fetch = [pltpu.make_async_copy(a, b, hsem.at[i]) for i, (a, b) in enumerate(loads)]
    for f in fetch:
        f.start()

    barrier = pltpu.get_barrier_semaphore()

    def greet(target):
        pl.semaphore_signal(barrier, inc=1, device_id=target, device_id_type=MESH)

    loop(1, 16, lambda k: greet(ring((p + k) & 15)))
    loop(1, 16, lambda k: greet(plane((h + k) & 15)))
    greet(yu)
    greet(yd)

    fetch[0].wait()
    fetch[1].wait()
    pf[...] = jnp.full((8, 256), -1000.0, F32)
    for a in range(2):
        pf[a : a + 1, 0:FACE] = pin[a].astype(F32)
    down = iota((FACE, FACE), 0).astype(F32)
    for a in range(2):
        onto = (pf[a : a + 1, 0:FACE] == down).astype(F32)
        snd[400 * a : 400 * a + FACE, :] = jnp.dot(onto, rv[a], precision=HIGHEST, preferred_element_type=F32)

    pl.semaphore_wait(barrier, 32)

    def face_copy(src, dst, turn, face):
        rows = pl.ds(FACE * face, FACE)
        return remote(src.at[rows], dst.at[rows], xs.at[turn], xr.at[turn], (xu, xd, yu, yd)[face])

    for a in range(2):
        remote(pf, pn.at[a], ps.at[0], pr.at[0], (xu, yu)[a]).start()
    for f in (0, 2):
        face_copy(snd, rx0, 0, f).start()
    lane = iota((8, 128), 1)
    mine = jnp.zeros((8, 128), F32)
    for z in range(2):
        base = core * 48 + z * 24 + gx * 3
        node = jnp.full((8, 128), inc[4 * z], jnp.int32)
        mine = jnp.where((lane >= base) & (lane < base + 3), (3 * node + (lane - base)).astype(F32), mine)
    idt[...] = mine
    idr[p] = mine

    fetch[2].wait()
    phf[...] = ph[...].astype(F32)
    fetch[3].wait()
    for k in range(12):
        packed[p, 6 * k : 6 * k + 6, :] = cin[:, 128 * k : 128 * k + 128]
    call[...] = jnp.zeros((16, 8, 1536), F32)

    full = iota((24, ORDER), 1)
    zone = jnp.where(full < SHARED, 1.0, jnp.where(full < SHARED + FACE, 0.0, ACTIVE_Z))
    pef[...] = jnp.zeros((120, ORDER), F32)
    pef[0:24, :] = phf[...] * zone
    r, m = iota((128, 128), 0), iota((128, 128), 1)
    block = (r * 683) >> 14
    e = r - 24 * block
    c = (e * 11) >> 5
    over = 1 + jnp.where(block == 1, 1, 0) - jnp.where(block == 2, 1, 0) + (c & 1)
    up = 1 + jnp.where(block == 3, 1, 0) - jnp.where(block == 4, 1, 0) + ((c >> 1) & 1)
    to = over * 24 + up * 6 + (c >> 2) * 3 + (e - 3 * c)
    place = ((to == m) & (r < 120)).astype(F32).astype(BF16)

    windows = ((0, 384), (128, 512), (384, 768), (512, 896))
    for blk, target in enumerate((xd, xu, yd, yu)):
        low, high = windows[blk]
        remote(phf.at[:, low:high], phn.at[blk, :, low:high], fs.at[0], fr.at[0], target).start()

    def far(step, size):
        return min(step, size - step)

    ring_steps = sorted(((dx, dc) for dx in range(8) for dc in (1, 0)), key=lambda d: -far(d[0], 8))
    ring_others = [2 * ((gx + dx) & 7) + ((core + dc) & 1) for dx, dc in ring_steps if dx or dc]
    plane_steps = sorted(
        ((dy, dx) for dy in range(4) for dx in range(4)), key=lambda d: -far(d[0], 4) - far(d[1], 4)
    )
    plane_others = [4 * (((h >> 2) + dy) & 3) + ((h + dx) & 3) for dy, dx in plane_steps if dy or dx]

    def started(me, where, src, dst, send, recv):
        for q in ring_others if where is ring else plane_others:
            remote(src(q), dst.at[me], send, recv, where(q)).start()

    def ended(dst, send, recv):
        all_blocks = remote(dst.at[0:15], dst.at[0:15], send, recv, xu)
        all_blocks.wait_recv()
        all_blocks.wait_send()

    other = device(gx, 2 * h + 1 - core)

    def rows_to(slot, target, turn):
        return remote(packed.at[slot], packed.at[slot], cs.at[turn], cr.at[turn], target)

    for k in (1, 7, 2, 6):
        rows_to(p, device((gx + k) & 7, gy), 0).start()
    rows_to(p, other, 2).start()
    started(p, ring, lambda q: idt, idr, ns.at[0], nr.at[0])

    def rows_in(count, turn):
        some = packed.at[0:count]
        arrived = remote(some, some, cs.at[turn], cr.at[turn], xu)
        arrived.wait_recv()
        arrived.wait_send()

    both_pairs = remote(pn, pn, ps.at[0], pr.at[0], xu)
    both_pairs.wait_recv()
    both_pairs.wait_send()
    for a, (up, low, shift) in enumerate(((FACE, 0, 0), (344, 144, 16))):
        wide = jnp.concatenate([pf[...], jnp.full((8, 384), -1000.0, F32)], axis=1)
        own = pltpu.roll(wide, up, 1)[a : a + 1, :]
        long = jnp.concatenate([pn[a], jnp.full((8, 256), -1000.0, F32)], axis=1)
        col = jnp.transpose(pltpu.roll(long, FACE + shift, 1))[:, a : a + 1]
        row = (iota((512, 640), 0) - shift).astype(F32)
        at_col = (iota((512, 640), 1) - low).astype(F32)
        px[a] = jnp.where((own == row) | (col == at_col), 1.0, 0.0).astype(BF16)

    def sent_x_rows(matrix, result):
        result[0:400, :] = dot(px[0, 0:400, :], matrix[0:640, :]).astype(BF16)

    def sent_y_rows(matrix, result):
        result[400:800, :] = dot(px[1, 16:416, :], matrix[256:896, :]).astype(BF16)

    def put(x, dst):
        high, low = halves(x)
        dst[:, 0:128] = high
        dst[:, 128:256] = low

    def joined(both):
        return both[:, 0:128] + both[:, 128:256]

    def product(matrix, chunks, result):
        def chunk(i):
            rows = pl.ds(pl.multiple_of(i * 400, 400), 400)
            result[rows, :] = joined(dot(matrix[rows, :], yb[...]))

        loop(0, chunks, chunk)

    def field(u, arrived, scale):
        return jnp.concatenate(
            [
                scale * (u[0:SHARED, :] - arrived[...]),
                jnp.zeros((FACE, LOADS), F32),
                (scale * ACTIVE_Z) * u[SHARED + FACE : ORDER, :],
            ],
            axis=0,
        )

    def total(a, b):
        return jnp.sum(a * b, axis=0, keepdims=True)

    def extras(*rows, size=8):
        sub = iota((size, 128), 0)
        tile = jnp.zeros((size, 128), F32)
        for i, row in enumerate(rows):
            tile = jnp.where(sub == i, row, tile)
        return tile

    def send_faces(src, dst, turn):
        for f in range(4):
            face_copy(src, dst, turn, f).start()

    def wait_faces(dst, turn):
        whole = remote(dst, dst, xs.at[turn], xr.at[turn], xu)
        whole.wait_recv()
        whole.wait_send()

    fetch[4].wait()
    sent_x_rows(sm, ss)

    half = remote(rx0.at[0:400], rx0.at[0:400], xs.at[0], xr.at[0], xu)
    half.wait_recv()
    half.wait_send()
    zeros = jnp.zeros((FACE, LOADS), F32)
    y0[...] = 0.5 * jnp.concatenate(
        [-rx0[0:FACE, :], rv[0], -rx0[2 * FACE : 3 * FACE, :], rv[1], zeros, ACTIVE_Z * rv[2]], axis=0
    )
    put(y0[...], yb)
    product(sm, 3, t0)
    start_energy = total(y0[...], t0[...])

    quarters = remote(phn.at[:, :, 0:384], phn.at[:, :, 0:384], fs.at[0], fr.at[0], xu)
    quarters.wait_recv()
    quarters.wait_send()
    at_lane = iota((24, 896), 1)
    blocks = []
    for blk in range(4):
        keep = (at_lane >= FACE * blk) & (at_lane < FACE * (blk + 1))
        blocks.append(jnp.where(keep, -phn[blk], 0.0))
    along_x = jnp.concatenate(blocks[0:2], axis=0)[:, 0:512].astype(BF16)
    along_y = jnp.concatenate(blocks[2:4], axis=0)[:, 384:896].astype(BF16)
    pef[24:72, 0:640] = dot(along_x, px[0])
    pef[72:120, 256:896] = dot(along_y, px[1])
    pe[...] = pef[...].astype(BF16)

    def corner_loads(t, result):
        put(t[...], tb)
        result[...] = 0.5 * joined(dot(pe[...], tb[...]))

    fetch[5].wait()
    corner_loads(t0, cl0)

    def coarse(turn, loads, tile, during_a, during_b, during_c, during_d):
        g = 4 * turn
        clt[...] = jnp.transpose(jnp.concatenate([loads, tile], axis=0))
        started(
            p, ring, lambda q: clt.at[pl.ds(pl.multiple_of(8 * q, 8), 8)], ra.at[turn], gs.at[0], gr.at[g]
        )
        ra[turn, p] = clt[pl.ds(pl.multiple_of(8 * p, 8), 8), :]
        during_a()
        ended(ra.at[turn], gs.at[0], gr.at[g])
        got = jnp.concatenate([ra[turn, i] for i in range(16)], axis=1)
        both = dot(stacked(got), at[...])
        mb[...] = both[0:8] + both[8:16]
        started(h, plane, lambda q: mb, rb.at[turn], gs.at[1], gr.at[g + 1])
        rb[turn, h] = mb[...]
        during_b()
        ended(rb.at[turn], gs.at[1], gr.at[g + 1])
        pieces, sums = [], jnp.zeros((8, 128), F32)
        for i in range(16):
            here, before, after = rb[turn, i], rb[turn, (i + 15) % 16], rb[turn, (i + 1) % 16]
            sums = sums + here[:, 0:128]
            part = jnp.where(lane < 96, here[:, 0:128] + before[:, 128:256], 0.0)
            part = part + jnp.where((lane >= 48) & (lane < 72), pltpu.roll(after[:, 0:128], 80, 1), 0.0)
            part = part + jnp.where((lane >= 72) & (lane < 96), pltpu.roll(after[:, 128:256], 104, 1), 0.0)
            pieces.append(part)
        four = lax.dot_general(
            stacked(jnp.concatenate(pieces, axis=1)), cp[...], NT, preferred_element_type=F32
        )
        sb[...] = joined(four[0:8]) + joined(four[8:16])
        started(h, plane, lambda q: sb, rc.at[turn], gs.at[0], gr.at[g + 2])
        rc[turn, h] = sb[...]
        during_c()
        ended(rc.at[turn], gs.at[0], gr.at[g + 2])
        got = jnp.concatenate([rc[turn, i] for i in range(16)], axis=1)
        both = dot(stacked(got), ohp[...])
        picked = both[0:8] + both[8:16]
        for q in range(16):
            first, by = divmod(24 * (q // 2), 128)
            at_tile = 384 * (q % 2) + 128 * first
            one = picked[:, at_tile : at_tile + 128]
            if by:
                two = picked[:, at_tile + 128 : at_tile + 256]
                one = jnp.where(lane < 128 - by, pltpu.roll(one, 128 - by, 1), pltpu.roll(two, 128 - by, 1))
            pb[q] = jnp.where(lane < 120, one, sums)
        started(p, ring, lambda q: pb.at[q], rd.at[turn], gs.at[1], gr.at[g + 3])
        rd[turn, p] = pb[p]
        during_d()
        ended(rd.at[turn], gs.at[1], gr.at[g + 3])
        solved = jnp.transpose(rd[turn].reshape(128, 128))
        high, low = halves(solved)
        corners = joined(dot(place, jnp.concatenate([high, low], axis=1)))
        return solved[120:128, :], corners

    def a0():
        rows_in(4, 0)
        below, above = 2 * ((gx + 6) & 7) + core, 2 * ((gx + 2) & 7) + core
        rows_to(below, xu, 1).start()
        rows_to(above, xd, 1).start()
        rows_to(below, device((gx + 2) & 7, gy), 1).start()
        sent_y_rows(sm, ss)
        product(ss, 2, ts)
        ended(idr, ns.at[0], nr.at[0])
        idm[...] = sum([idr[i] for i in range(1, 16)], idr[0])
        started(h, plane, lambda q: idm, ids, ns.at[1], nr.at[1])
        ids[h] = idm[...]
        fetch[6].wait()
        sent_x_rows(km, ks)
        sent_y_rows(km, ks)

    def b0():
        rows_in(3, 1)
        for k in range(1, 8):
            rows_to(2 * ((gx + k) & 7) + core, other, 2).start()
        send_faces(ts, rx1, 1)
        rows_in(8, 2)
        for slot in range(16):
            for k in range(12):
                call[slot, 0:6, 128 * k : 128 * k + 128] = packed[slot, 6 * k : 6 * k + 6, :]
        high, low = halves(call[...].reshape(128, 1536))
        c256[0:128, :] = high
        c256[128:256, :] = low
        ended(ids, ns.at[1], nr.at[1])
        row = iota((1536, 256), 0)
        lanes = iota((1, 128), 1)

        def columns(j):
            pair_ids = [jnp.where(lanes < 96, ids[2 * j + s][0:1, :], -1.0) for s in range(2)]
            wanted = jnp.concatenate(pair_ids, axis=1).astype(jnp.int32)
            pick = (row == wanted).astype(F32).astype(BF16)
            cp[:, pl.ds(pl.multiple_of(j * 256, 256), 256)] = dot(c256[...], pick).astype(BF16)

        loop(0, 8, columns)

    def direction(t, arrived, w, turn, result):
        wait_faces(arrived, turn)
        w[...] = field(t, arrived, 0.5)
        put(w[...], yb)
        product(ks, 2, ts)
        send_faces(ts, result, turn + 1)
        return joined(dot(ph[...], yb[...]))

    kept = {}

    def c0():
        kept["w0"] = direction(t0, rx1, w0, 1, rx2)
        nearby = jnp.concatenate([ids[(h + 15) & 15], ids[h], ids[(h + 1) & 15]], axis=1)
        fetch[7].wait()
        found = dot(stacked(nearby), ot[...])
        wanted = (found[0:1] + found[8:9]).astype(jnp.int32)

        def picks(j):
            rr = iota((128, 768), 0)
            own = 192 * (rr >> 4) + 12 * j + 6 * ((rr >> 3) & 1) + (rr & 7)
            own = jnp.where((rr & 7) < 6, own, -2)
            ohp[pl.ds(pl.multiple_of(j * 128, 128), 128), :] = (own == wanted).astype(F32).astype(BF16)

        loop(0, 16, picks)
        pet[...] = jnp.transpose(jnp.concatenate([pef[...], jnp.zeros((8, ORDER), F32)], axis=0)).astype(BF16)

        def chunk(i):
            rows = pl.ds(pl.multiple_of(i * 400, 400), 400)
            tp[rows, :] = dot(sm[rows, :], pet[...])

        loop(0, 3, chunk)

    def operator():
        put(tp[...], tb)
        through = 0.25 * joined(dot(pe[...], tb[...]))
        through = jnp.concatenate([through, jnp.zeros((8, 128), F32)], axis=0)
        high, low = halves(through)
        big[:, 0:128] = high
        big[:, 128:256] = low

    def second(d, arrived, turn, result):
        wait_faces(arrived, turn)
        yp[...] = field(d, arrived, 0.5)
        put(yp[...], yb)
        product(sm, 3, tp)
        corner_loads(tp, result)

    def coupled(corners):
        high, low = halves(corners)
        wide = jnp.concatenate([high, low], axis=1)
        return joined(dot(big[...], jnp.concatenate([wide, wide], axis=0)))[0:120]

    def d_first():
        product(km, 3, d0)
        operator()
        second(d0, rx2, 2, clm)
        kept["c00"] = total(w0[...], d0[...])
        kept["k1"] = total(t0[...], yp[...])
        kept["k2"] = total(yp[...], tp[...])

    sums, g0 = coarse(0, cl0[...], extras(start_energy), a0, b0, c0, d_first)
    start_energy = sums[0:1, :]
    g0x = g0[0:120]
    cl1[...] = clm[...] + coupled(g0)
    c00 = kept["c00"] + total(kept["w0"], g0[0:24])
    k1 = kept["k1"] + total(cl0[...], g0x)
    k2 = kept["k2"] + total(clm[...] + cl1[...], g0x)

    def a1():
        high, low = halves(0.5 * g0)
        yq[...] = yp[...] + joined(dot(pet[...], jnp.concatenate([high, low], axis=1)))
        put(yq[...], yb)
        product(ss, 2, ts)
        send_faces(ts, rx3, 3)
        product(sm, 3, tq)

    def b1():
        kept["wm"] = direction(tq, rx3, wm, 3, rx4)
        product(km, 3, dm)
        kept["c01"] = total(w0[...], dm[...])
        kept["c10"] = total(wm[...], d0[...]) + total(kept["wm"], g0[0:24])
        kept["c11"] = total(wm[...], dm[...])

    def c1():
        second(dm, rx4, 4, clm)
        kept["m1"] = total(t0[...], yp[...])
        kept["m2"] = total(tq[...], yp[...])
        kept["m3"] = total(yp[...], tp[...])

    sums, gm = coarse(1, cl1[...], extras(c00, k1, k2), a1, b1, c1, lambda: None)
    gmx = gm[0:120]
    alpha = start_energy / sums[0:1, :]
    energy = start_energy - 2.0 * alpha * sums[1:2, :] + alpha * alpha * sums[2:3, :]
    ratio = 1.0 + energy / start_energy
    c01 = kept["c01"] + kept["c10"] + total(kept["w0"], gm[0:24])
    c11 = kept["c11"] + total(kept["wm"], gm[0:24])
    m1 = kept["m1"] + total(cl0[...], gmx)
    m2 = kept["m2"] + total(cl1[...], gmx)
    m3 = kept["m3"] + total(2.0 * clm[...] + coupled(gm), gmx)
    curvature = ratio * ratio * c00 - ratio * alpha * c01 + alpha * alpha * c11
    cross = ratio * (k1 - alpha * k2) - alpha * (m1 - alpha * m2)
    square = ratio * ratio * k2 - 2.0 * ratio * alpha * m2 + alpha * alpha * m3
    fb0[...] = extras(curvature, cross, square, size=4)
    started(p, ring, lambda q: fb0, fb1, gs.at[0], gr.at[8])
    fb1[p] = fb0[...]
    ended(fb1, gs.at[0], gr.at[8])
    fb2[...] = sum([fb1[i] for i in range(1, 16)], fb1[0])
    started(h, plane, lambda q: fb2, fb3, gs.at[1], gr.at[9])
    fb3[h] = fb2[...]
    ended(fb3, gs.at[1], gr.at[9])
    sums = sum([fb3[i] for i in range(1, 16)], fb3[0])
    step = energy / sums[0:1, :]
    final = energy - 2.0 * step * sums[1:2, :] + step * step * sums[2:3, :]
    red[...] = final / start_energy
    for a in range(3):
        rows = slice(FACE * (2 * a + 1), FACE * (2 * a + 2))
        out[a] = (alpha + step * ratio) * w0[rows, :] - (step * alpha) * wm[rows, :]


def local(rhs, stiff, schur, phi, coarse, inc, pair):
    table, order = jnp.asarray(assembly_table(), BF16), jnp.asarray(order_table(), BF16)
    v = pltpu.VMEM
    wide, sent = v((ORDER, LOADS), F32), v((SHARED, LOADS), F32)
    dma = pltpu.SemaphoreType.DMA
    tile, group = v((8, 128), F32), v((16, 8, 128), F32)
    scratch = [
        v((3, FACE, LOADS), F32), v((ORDER, ORDER), BF16), v((ORDER, ORDER), BF16),
        v((SHARED, ORDER), BF16), v((SHARED, ORDER), BF16),
        v((24, ORDER), BF16), v((24, ORDER), F32), v((4, 24, 896), F32),
        v((6, 1536), F32), v((16, 72, 128), F32), v((16, 8, 1536), F32), v((3, 1, FACE), jnp.int32), v((8, 256), F32), v((2, 8, 256), F32),
        v((2048, 256), BF16), v((384, 768), BF16),
        v((ORDER, 256), BF16), v((ORDER, 256), BF16),
        sent, sent, sent, sent, sent, sent, sent,
        wide, wide, wide, wide, wide, wide, wide, wide, wide, wide,
        v((2, 512, 640), BF16), v((120, ORDER), F32), v((120, ORDER), BF16), v((ORDER, 128), BF16),
        v((128, 256), BF16), v((128, 128), F32), v((120, 128), F32), v((120, 128), F32), v((120, 128), F32),
        v((2, 16, 8, 128), F32), v((8, 256), F32), v((2, 16, 8, 256), F32),
        tile, v((2, 16, 8, 128), F32), group, v((2, 16, 8, 128), F32),
        v((256, 2048), BF16), v((256, 1536), BF16), v((2048, 768), BF16),
        tile, group, tile, group,
        v((4, 128), F32), v((16, 4, 128), F32), v((4, 128), F32), v((16, 4, 128), F32),
        dma((8,)), dma((5,)), dma((5,)), dma((1,)), dma((1,)), dma((1,)), dma((1,)),
        dma((2,)), dma((2,)), dma((3,)), dma((3,)), dma((2,)), dma((10,)),
    ]
    any_space = pl.BlockSpec(memory_space=pl.ANY)
    in_vmem = pl.BlockSpec(memory_space=pltpu.VMEM)
    result, reduction = pl.pallas_call(
        kernel,
        out_shape=(v((3, FACE, LOADS), F32), v((1, LOADS), F32)),
        in_specs=[any_space] * 5 + [pl.BlockSpec(memory_space=pltpu.SMEM)] + [any_space] * 3,
        out_specs=(in_vmem, in_vmem),
        scratch_shapes=scratch,
        compiler_params=pltpu.CompilerParams(
            collective_id=0, has_side_effects=True, vmem_limit_bytes=60 * 1024 * 1024
        ),
        name="domain_decomposition",
    )(
        rhs[0, 0, 0], stiff[0, 0, 0], schur[0, 0, 0], phi[0, 0, 0], coarse, inc[0, 0, 0],
        pair.reshape(3, 1, FACE), table, order,
    )
    return result[None, None, None], reduction[0]


def solution(mesh):
    four = P("gx", "gy", None, None)
    five = P("gx", "gy", None, None, None)
    six = P("gx", "gy", None, None, None, None)
    return jax.shard_map(
        local,
        mesh=mesh,
        in_specs=(six, five, five, five, P(("gx", "gy"), None), four, five),
        out_specs=(six, P()),
        check_vma=False,
    )
```
